128 devices in a mesh: data: 1, time: 128 (over z, y, x, core).
Axes of the slice: x: 4, y: 4, z: 4, core: 2. Of those that a mesh axis runs over, the one named last changes fastest.
Arguments:
- x_init: float32 [64, 16, 10], P('data')
- w_in: bfloat16 [10, 256], replicated
- w_out: bfloat16 [256, 10], replicated
- mod_scale: bfloat16 [2048, 256], P('time')
- mod_shift: bfloat16 [2048, 256], P('time')
- step_size: float32 [2048], P('time')
Outputs:
- output: float32 [2048, 64, 16, 10], P('time', 'data')
All inputs are finite; a program needn't handle non-finite values.
Results may differ from the reference program's by a relative error of at most 0.001.
Values are sent between devices in bfloat16 or wider.
A program may use at most 1 GiB of HBM per device.

```python
import jax
import jax.numpy as jnp
from jax import lax

BATCH = 64
TOKENS = 16
CHANNELS = 10
HIDDEN = 256
STEPS = 2048
SWEEPS = 4


def setup_inputs(seed: int = 0, part: int = 0) -> dict:
    key_list = jax.random.split(jax.random.key(seed), 7)
    x_init = jax.random.normal(jax.random.fold_in(key_list[0], part), (BATCH, TOKENS, CHANNELS), jnp.float32)
    w_in = jax.random.normal(key_list[1], (CHANNELS, HIDDEN), jnp.float32) * (CHANNELS * STEPS) ** -0.5
    w_raw = jax.random.normal(key_list[2], (HIDDEN, CHANNELS), jnp.float32)
    w_out = (w_raw - jnp.mean(w_raw, axis=0, keepdims=True)) * (1.5 * HIDDEN ** -0.5)
    time_pos = (jnp.arange(STEPS, dtype=jnp.float32) + 0.5) / STEPS
    mode_coef = 0.4 * jax.random.normal(key_list[3], (3, HIDDEN), jnp.float32)
    mod_scale = (mode_coef[0][None, :] + mode_coef[1][None, :] * jnp.cos(jnp.pi * time_pos)[:, None] + mode_coef[2][None, :] * jnp.cos(2.0 * jnp.pi * time_pos)[:, None] + 0.1 * jax.random.normal(key_list[4], (STEPS, HIDDEN), jnp.float32))
    mod_shift = jax.random.normal(key_list[5], (STEPS, HIDDEN), jnp.float32)
    step_size = jax.random.uniform(key_list[6], (STEPS,), jnp.float32, 0.5, 1.5) * STEPS ** -0.5
    return {"x_init": x_init, "w_in": w_in.astype(jnp.bfloat16), "w_out": w_out.astype(jnp.bfloat16), "mod_scale": mod_scale.astype(jnp.bfloat16), "mod_shift": mod_shift.astype(jnp.bfloat16), "step_size": step_size}


def denoise(latent, w_in, w_out, scale_row, shift_row):
    flat_in = latent.astype(jnp.bfloat16).reshape(-1, latent.shape[-1])
    pre_act = jnp.dot(flat_in, w_in, preferred_element_type=jnp.float32)
    hidden_act = jax.nn.gelu(pre_act * (1.0 + scale_row.astype(jnp.float32)) + shift_row.astype(jnp.float32), approximate=True)
    return jnp.dot(hidden_act.astype(jnp.bfloat16), w_out, preferred_element_type=jnp.float32).reshape(latent.shape)


def reference(x_init, w_in, w_out, mod_scale, mod_shift, step_size):
    def one_step_drift(item):
        return denoise(item[0], w_in, w_out, item[1], item[2])

    def one_sweep(latents, unused):
        drifts = lax.map(one_step_drift, (latents, mod_scale, mod_shift))
        increments = step_size[:-1, None, None, None] * (0.5 * (drifts[:-1] + drifts[1:]))
        running = jnp.cumsum(increments, axis=0)
        return jnp.concatenate([x_init[None], x_init[None] + running], axis=0), unused

    start = jnp.broadcast_to(x_init[None], (STEPS,) + x_init.shape)
    final, unused_out = lax.scan(one_sweep, start, None, length=SWEEPS)
    return final
```

```python
import functools

import jax
import jax.numpy as jnp
from jax import lax
from jax.experimental import pallas as pl
from jax.experimental.pallas import tpu as pltpu
from jax.sharding import PartitionSpec as P

CUBE = 0.044715
ROOT = 0.7978845608028654
F32, BF16 = jnp.float32, jnp.bfloat16

def nn(a, b):
    return lax.dot_general(a, b, (((1,), (0,)), ((), ())), preferred_element_type=F32)

def act(y):
    q = y * ((2.0 * ROOT) + (8.0 * ROOT * CUBE) * (y * y))
    return (y + y * jnp.tanh(q)).astype(BF16)

def body(ms, mt, hs, x0, xr, wi, wo, tri, out, sf, bf, xrow, db, *accs, scan_u=8):
    ys, ds, es = accs[:4], accs[4:8], accs[8:]
    db[128] = jnp.zeros((16, 128), F32)
    xrow[...] = jnp.zeros_like(xrow)
    x0v = x0[...]
    wov = wo[...]

    def conv(i, _):
        r = pl.ds(pl.multiple_of(i * 64, 64), 64)
        sf[r, :] = 0.5 + 0.5 * ms[r, :].astype(F32)
        bf[r, :] = 0.5 * mt[r, :].astype(F32)
        return 0
    lax.fori_loop(0, 32, conv, 0)

    def rowpair(ref, r):
        a = jnp.broadcast_to(ref[pl.ds(r, 1), :], (8, 256))
        b = jnp.broadcast_to(ref[pl.ds(r + 1, 1), :], (8, 256))
        return jnp.concatenate([a, b], axis=0)

    def hidden(t, y_of):
        hs_ = []
        for k in range(16):
            r = t * 32 + 2 * k
            hs_.append(act(y_of(k) * rowpair(sf, r) + rowpair(bf, r)))
        return jnp.concatenate(hs_, axis=0)

    def put(t, d):
        db[2 * t] = d[:, :128]
        db[2 * t + 1] = d[:, 128:]

    def xt(t):
        v = xrow[pl.ds(pl.multiple_of(t * 256, 256), 256), :]
        return jnp.concatenate([v, jnp.zeros((256, 128), BF16)], axis=1)

    for r in accs:
        pltpu.matmul_pop(r)
    pltpu.matmul_push_rhs(wi[...], staging_register=0, mxu_index=0)
    pltpu.matmul_acc_lhs(ys[0], xr[...], load_staged_rhs=0)
    u = pltpu.matmul_pop(ys[0])[:8]

    def sweep(first):
        if not first:
            pltpu.matmul_push_rhs(wi[...], staging_register=0, mxu_index=0)
            pltpu.matmul_acc_lhs(ys[0], xt(0), load_staged_rhs=0)
            pltpu.matmul_acc_lhs(ys[1], xt(1))
        def step(i, _):
            for s in range(4):
                t = 4 * i + s
                if first:
                    uu = jnp.concatenate([u, u], axis=0)
                    h = hidden(t, lambda k: uu)
                else:
                    pltpu.matmul_acc_lhs(ys[(s + 2) % 4], xt(jnp.minimum(t + 2, 63)))
                    y = pltpu.matmul_pop(ys[s])
                    h = hidden(t, lambda k: y[16 * k:16 * k + 16])
                pltpu.matmul_push_rhs(h, staging_register=s % 2, mxu_index=1, transpose=True)
                pltpu.matmul_acc_lhs(ds[s], wov, load_staged_rhs=s % 2)
                put(lax.rem(t + 62, 64), pltpu.matmul_pop(ds[(s + 2) % 4]))
            return 0
        lax.fori_loop(0, 16, step, 0)
        put(62, pltpu.matmul_pop(ds[2]))
        put(63, pltpu.matmul_pop(ds[3]))
        if not first:
            pltpu.matmul_pop(ys[0])
            pltpu.matmul_pop(ys[1])

    lane = lax.broadcasted_iota(jnp.int32, (16, 128), 1)
    zb = jnp.zeros((16, 128), BF16)
    def scan(last):
        pltpu.matmul_push_rhs(tri[...], staging_register=0, mxu_index=1)
        def feed(k, e, load=None):
            for i in range(8):
                t = k * 8 + i
                d = db[t]
                dn = jnp.where(lane < 120, pltpu.roll(d, 120, 1), pltpu.roll(db[t + 1], 120, 1))
                g = (d + dn) * hs[pl.ds(t, 1), :]
                hi = g.astype(BF16)
                r1 = g - hi.astype(F32)
                mid = r1.astype(BF16)
                lo = (r1 - mid.astype(F32)).astype(BF16)
                pltpu.matmul_acc_lhs(e[i], jnp.concatenate([hi, mid], axis=1), load_staged_rhs=load if i == 0 else None)
                pltpu.matmul_acc_lhs(e[i], jnp.concatenate([lo, zb], axis=1))
        def drain(k, e, carry):
            for i in range(8):
                t = k * 8 + i
                pr = pltpu.matmul_pop(e[i])
                x = carry + pr[:, :128]
                carry = carry + pr[:, 128:]
                if last:
                    out[t] = x
                else:
                    xrow[pl.ds(pl.multiple_of(t * 128, 128), 128), 0:16] = x.T.astype(BF16)
            return carry
        feed(0, es[:8], 0)
        def step(k, carry):
            feed(2 * k + 1, es[8:])
            carry = drain(2 * k, es[:8], carry)
            feed(jnp.minimum(2 * k + 2, 15), es[:8])
            return drain(2 * k + 1, es[8:], carry)
        lax.fori_loop(0, 8, step, x0v)
        for e in es[:8]:
            pltpu.matmul_pop(e)

    sweep(True)
    for _ in range(3):
        scan(False)
        sweep(False)
    scan(True)

def kernel(*refs, **kw):
    pl.run_scoped(functools.partial(body, *refs, **kw),
                  *[pltpu.ACC(0)((256, 256), F32)] * 4, *[pltpu.ACC(1)((16, 256), F32)] * 20)

def call(ms, mt, hs, x0, xr, wi, wo, tri, **kw):
    v = pl.BlockSpec(memory_space=pltpu.VMEM)
    return pl.pallas_call(
        functools.partial(kernel, **kw),
        out_shape=jax.ShapeDtypeStruct((128, 16, 128), F32),
        in_specs=[v] * 8, out_specs=v,
        scratch_shapes=[
            pltpu.VMEM((2048, 256), F32), pltpu.VMEM((2048, 256), F32),
            pltpu.VMEM((16384, 128), BF16), pltpu.VMEM((129, 16, 128), F32)],
        compiler_params=pltpu.CompilerParams(vmem_limit_bytes=60 * 2**20),
    )(ms, mt, hs, x0, xr, wi, wo, tri)


def triangle():
    i = jnp.arange(128)
    same = (i[:, None] % 8) == (i[None, :] % 8)
    strict = same & ((i[:, None] // 8) < (i[None, :] // 8))
    t = 256.0 * jnp.concatenate([strict, same], axis=1).astype(F32)
    return jnp.concatenate([t, t], axis=0).astype(BF16)

def untangle(src, out):
    for c in range(10):
        for half in range(2):
            m = src[half, :, c, :].T
            for k in range(16):
                out[k, c, 8 * half:8 * half + 8, :] = m[8 * k:8 * k + 8, :]

def solution(mesh):
    def local(x_init, w_in, w_out, mod_scale, mod_shift, step_size):
        me = lax.axis_index("time")
        half, batch = me // 64, me % 64
        xr = lax.dynamic_slice(x_init, (batch, half * 8, 0), (1, 8, 10))[0]
        ms = lax.all_gather(mod_scale, "time", axis=0, tiled=True)
        mt = lax.all_gather(mod_shift, "time", axis=0, tiled=True)
        st = lax.all_gather(step_size, "time", axis=0, tiled=True)
        x0 = jnp.pad(jnp.tile(xr.T, (1, 16)), ((0, 6), (0, 0)))
        xp = jnp.pad(xr, ((0, 248), (0, 246))).astype(BF16)
        wi = jnp.pad(w_in, ((0, 246), (0, 0)))
        wo = jnp.pad(w_out.T, ((0, 6), (0, 0)))
        hs = jnp.repeat(st * (0.5 / 256.0), 8).reshape(128, 128)
        mine = call(ms, mt, hs, x0, xp, wi, wo, triangle())
        got = lax.all_to_all(mine, "time", 0, 0, tiled=True)
        v = pl.BlockSpec(memory_space=pltpu.VMEM)
        res = pl.pallas_call(untangle, out_shape=jax.ShapeDtypeStruct((16, 10, 16, 64), F32), in_specs=[v], out_specs=v)(got.reshape(2, 64, 16, 128))
        return jnp.transpose(res, (0, 3, 2, 1))

    return jax.shard_map(local, mesh=mesh, in_specs=(P("data"), P(), P(), P("time"), P("time"), P("time")), out_specs=P("time", "data"), check_vma=False)
```

```python
import functools

import jax
import jax.numpy as jnp
from jax import lax
from jax.experimental import pallas as pl
from jax.experimental.pallas import tpu as pltpu
from jax.sharding import PartitionSpec as P

MESH = pl.DeviceIdType.MESH
CUBE = 0.044715
ROOT = 0.7978845608028654
F32, BF16 = jnp.float32, jnp.bfloat16

def nn(a, b):
    return lax.dot_general(a, b, (((1,), (0,)), ((), ())), preferred_element_type=F32)

def act(y):
    q = y * ((2.0 * ROOT) + (8.0 * ROOT * CUBE) * (y * y))
    return (y + y * jnp.tanh(q)).astype(BF16)

def body(buf, hs, xt_, w_in, w_out, out, sf, bf, xrow, db, wi, wo, tris, *accs):
    ys, ds, es = accs[:4], accs[4:8], accs[8:24]
    u_acc = accs[24]
    db[128] = jnp.zeros((16, 128), F32)
    xrow[...] = jnp.zeros_like(xrow)
    me = lax.axis_index("time")
    core = me % 2
    half, batch = me // 64, me % 64
    wi[...] = jnp.zeros_like(wi)
    wo[...] = jnp.zeros_like(wo)
    wi[0:10, :] = w_in[...]
    wo[0:10, :] = w_out[...]
    lane8 = lax.broadcasted_iota(jnp.int32, (8, 128), 1)
    pick = lax.broadcasted_iota(jnp.int32, (8, 64), 1) == batch
    xr = jnp.zeros((8, 128), F32)
    for ch in range(10):
        col = jnp.sum(jnp.where(pick, xt_[ch, pl.ds(pl.multiple_of(half * 8, 8), 8), :], 0.0), axis=1, keepdims=True)
        xr = jnp.where(lane8 == ch, col, xr)
    x0v = jnp.concatenate([xr] * 16, axis=0).T[0:16, :]
    xl = jnp.concatenate([jnp.concatenate([xr, jnp.zeros((8, 128), F32)], axis=0).astype(BF16), jnp.zeros((16, 128), BF16)], axis=1)
    ri = lax.broadcasted_iota(jnp.int32, (256, 256), 0) % 128
    ci = lax.broadcasted_iota(jnp.int32, (256, 256), 1)
    cm = ci % 128
    tri = jnp.where(((ri % 8) == (cm % 8)) & ((ci >= 128) | ((ri // 8) < (cm // 8))), 256.0, 0.0).astype(BF16)
    tris[...] = tri
    for r in accs:
        pltpu.matmul_pop(r)
    pltpu.matmul_push_rhs(wi[...], staging_register=0, mxu_index=1)
    pltpu.matmul_acc_lhs(u_acc, xl, load_staged_rhs=0)
    u = pltpu.matmul_pop(u_acc)[:8]
    wov = wo[...]

    def other(t):
        return (t % 4) * 16 + ((t // 4) % 4) * 4 + t // 16

    def conv(t, _):
        r = pl.ds(pl.multiple_of(t * 32, 32), 32)
        sf[r, :] = 0.5 + 0.5 * buf[0, t].astype(F32)
        bf[r, :] = 0.5 * buf[1, other(t)].astype(F32)
        return 0
    lax.fori_loop(0, 64, conv, 0)

    def rowpair(ref, r):
        a = jnp.broadcast_to(ref[pl.ds(r, 1), :], (8, 256))
        b = jnp.broadcast_to(ref[pl.ds(r + 1, 1), :], (8, 256))
        return jnp.concatenate([a, b], axis=0)

    def hidden(t, y_of):
        hs_ = []
        for k in range(16):
            r = t * 32 + 2 * k
            hs_.append(act(y_of(k) * rowpair(sf, r) + rowpair(bf, r)))
        return jnp.concatenate(hs_, axis=0)

    def put(t, d):
        db[2 * t] = d[:, :128]
        db[2 * t + 1] = d[:, 128:]

    def xt(t):
        v = xrow[pl.ds(pl.multiple_of(t * 256, 256), 256), :]
        return jnp.concatenate([v, jnp.zeros((256, 128), BF16)], axis=1)

    def sweep(first):
        if not first:
            pltpu.matmul_push_rhs(wi[...], staging_register=0, mxu_index=0)
            pltpu.matmul_acc_lhs(ys[0], xt(0), load_staged_rhs=0)
            pltpu.matmul_acc_lhs(ys[1], xt(1))
        def step(i, _):
            for s in range(4):
                t = 4 * i + s
                if first:
                    uu = jnp.concatenate([u, u], axis=0)
                    h = hidden(t, lambda k: uu)
                else:
                    pltpu.matmul_acc_lhs(ys[(s + 2) % 4], xt(jnp.minimum(t + 2, 63)))
                    y = pltpu.matmul_pop(ys[s])
                    h = hidden(t, lambda k: y[16 * k:16 * k + 16])
                pltpu.matmul_push_rhs(h, staging_register=s % 2, mxu_index=1, transpose=True)
                pltpu.matmul_acc_lhs(ds[s], wov, load_staged_rhs=s % 2)
                put(lax.rem(t + 62, 64), pltpu.matmul_pop(ds[(s + 2) % 4]))
            return 0
        lax.fori_loop(0, 16, step, 0)
        put(62, pltpu.matmul_pop(ds[2]))
        put(63, pltpu.matmul_pop(ds[3]))
        if not first:
            pltpu.matmul_pop(ys[0])
            pltpu.matmul_pop(ys[1])

    lane = lax.broadcasted_iota(jnp.int32, (16, 128), 1)
    zb = jnp.zeros((16, 128), BF16)
    def scan(last):
        pltpu.matmul_push_rhs(tris[...], staging_register=0, mxu_index=1)
        def feed(k, e, load=None):
            for i in range(8):
                t = k * 8 + i
                tile = k * 4 + i // 2
                tile = tile + core * (other(tile) - tile)
                d = db[t]
                dn = jnp.where(lane < 120, pltpu.roll(d, 120, 1), pltpu.roll(db[t + 1], 120, 1))
                g = (d + dn) * hs[tile, i % 2]
                hi = g.astype(BF16)
                r1 = g - hi.astype(F32)
                mid = r1.astype(BF16)
                lo = (r1 - mid.astype(F32)).astype(BF16)
                pltpu.matmul_acc_lhs(e[i], jnp.concatenate([hi, mid], axis=1), load_staged_rhs=load if i == 0 else None)
                pltpu.matmul_acc_lhs(e[i], jnp.concatenate([lo, zb], axis=1))
        def drain(k, e, carry):
            for i in range(8):
                t = k * 8 + i
                pr = pltpu.matmul_pop(e[i])
                x = carry + pr[:, :128]
                carry = carry + pr[:, 128:]
                if last:
                    out[t] = x
                else:
                    xrow[pl.ds(pl.multiple_of(t * 128, 128), 128), 0:16] = x.T.astype(BF16)
            return carry
        feed(0, es[:8], 0)
        def step(k, carry):
            feed(2 * k + 1, es[8:])
            carry = drain(2 * k, es[:8], carry)
            feed(jnp.minimum(2 * k + 2, 15), es[:8])
            return drain(2 * k + 1, es[8:], carry)
        lax.fori_loop(0, 8, step, x0v)
        for e in es[:8]:
            pltpu.matmul_pop(e)

    sweep(True)
    for _ in range(3):
        scan(False)
        sweep(False)
    scan(True)

def kernel(*refs, **kw):
    pl.run_scoped(functools.partial(body, *refs, **kw),
                  *[pltpu.ACC(0)((256, 256), F32)] * 4, *[pltpu.ACC(1)((16, 256), F32)] * 20, pltpu.ACC(1)((16, 256), F32))


def gather_kernel(ms, mt, st, buf, hs, own, hrow, sx, rx, sh, rh, sm, rm, sd, rd):
    me = lax.axis_index("time")
    core = me % 2
    x, y, z = (me // 2) % 4, (me // 8) % 4, me // 32
    a = x + core * (z - x)
    b = y
    c = z + core * (x - z)
    ka, kc = 1 + 15 * core, 16 - 15 * core

    def dev(da, db, dc):
        aa, bb, cc = (a + da) % 4, (b + db) % 4, (c + dc) % 4
        return 2 * (aa * ka + bb * 4 + cc * kc) + core

    def idx(da, db, dc):
        return ((c + dc) % 4) * 16 + ((b + db) % 4) * 4 + (a + da) % 4

    partner = me + 1 - 2 * core
    peers = [dev(1, 0, 0), dev(3, 0, 0), dev(2, 0, 0), dev(0, 1, 0), dev(0, 3, 0), dev(0, 2, 0),
             dev(0, 0, 1), dev(0, 0, 3), dev(0, 0, 2), partner]
    own[0] = ms[...]
    own[1] = mt[...]
    lane = lax.broadcasted_iota(jnp.int32, (1, 128), 1)
    row = jnp.zeros((1, 128), F32)
    for k in range(16):
        row = jnp.where(lane // 8 == k, st[k] * (0.5 / 256.0), row)
    hrow[...] = row

    barrier = pltpu.get_barrier_semaphore()
    for p in peers:
        pl.semaphore_signal(barrier, inc=1, device_id={"time": p}, device_id_type=MESH)
    pl.semaphore_wait(barrier, len(peers))

    def remote(src, dst, s, r, p):
        cp = pltpu.make_async_remote_copy(src_ref=src, dst_ref=dst, send_sem=s, recv_sem=r,
                                          device_id={"time": p}, device_id_type=MESH)
        cp.start()
        return cp

    mine = idx(0, 0, 0)
    sent = []
    half = pl.ds(pl.multiple_of(core * 16, 16), 16)
    other = pl.ds(pl.multiple_of(16 - core * 16, 16), 16)
    ex = remote(own.at[1 - core], buf.at[1 - core, idx_of(me, 1 - core), half], sx.at[0], rx.at[0], partner)
    hx = remote(hrow, hs.at[idx_of(me, 1 - core), core], sx.at[1], rx.at[1], partner)
    l1 = pltpu.make_async_copy(own.at[core], buf.at[core, mine, half], sx.at[2])
    l2 = pltpu.make_async_copy(hrow, hs.at[mine, core], sx.at[3])
    l1.start(); l2.start()
    ex.wait(); hx.wait(); l1.wait(); l2.wait()

    nsend = [0]
    def send(i, p):
        k = nsend[0]
        nsend[0] += 1
        sent.append(remote(buf.at[core, i], buf.at[core, i], sm.at[k], rm.at[i], p))
    def relay(i, k):
        sent.append(remote(buf.at[core, i], buf.at[core, i], sd.at[k], rd.at[i], partner))
    def arrive(i):
        pltpu.make_async_copy(buf.at[core, i], buf.at[core, i], rm.at[i]).wait()

    hn = [0]
    def hsend(ref, j, p):
        k = hn[0]
        hn[0] += 1
        sent.append(remote(ref, ref, sh.at[k], rh.at[k], p))
    def harrive(ref, k):
        pltpu.make_async_copy(ref, ref, rh.at[k]).wait()

    order = (0, 1, 3, 2)
    for d in order[1:]:
        send(mine, dev(d, 0, 0))
    hm = hs.at[mine]
    for d in order[1:]:
        hsend(hm, d, dev(d, 0, 0))
    relay(mine, 0)
    nrel = 1
    for da in order:
        i = idx(da, 0, 0)
        if da:
            arrive(i)
        for d in order[1:]:
            send(i, dev(0, d, 0))
        for d in (1, 3):
            send(i, dev(0, 0, d))
        if da:
            relay(i, nrel)
            nrel += 1
    for k, d in enumerate(order[1:]):
        harrive(hs.at[idx(-d % 4, 0, 0)], k)
    hb = hs.at[pl.ds(pl.multiple_of(c * 16 + b * 4, 4), 4)]
    for d in order[1:]:
        hsend(hb, d, dev(0, d, 0))
    for db in order[1:]:
        for da in order:
            i = idx(da, db, 0)
            arrive(i)
            for d in (1, 3):
                send(i, dev(0, 0, d))
            relay(i, nrel)
            nrel += 1
    for k, d in enumerate(order[1:]):
        harrive(hs.at[pl.ds(pl.multiple_of(c * 16 + ((b - d) % 4) * 4, 4), 4)], 3 + k)
    hc = hs.at[pl.ds(pl.multiple_of(c * 16, 16), 16)]
    for d in order[1:]:
        hsend(hc, d, dev(0, 0, d))
    n = 0
    for db in order:
        for da in order:
            for dc, step in ((3, 1), (1, 3)):
                i = idx(da, db, dc)
                arrive(i)
                if (n < 8) == (step == 1):
                    send(i, dev(0, 0, step))
                relay(i, nrel)
                nrel += 1
            n += 1
    for db in order:
        for da in order:
            i = idx(da, db, 2)
            arrive(i)
            relay(i, nrel)
            nrel += 1
    for k, d in enumerate(order[1:]):
        harrive(hs.at[pl.ds(pl.multiple_of(((c - d) % 4) * 16, 16), 16)], 6 + k)
    for i in range(64):
        pltpu.make_async_copy(buf.at[1 - core, i], buf.at[1 - core, i], rd.at[i]).wait()
    for cp in sent:
        cp.wait_send()


def idx_of(me, core):
    x, y, z = (me // 2) % 4, (me // 8) % 4, me // 32
    a, c = x + core * (z - x), z + core * (x - z)
    return c * 16 + y * 4 + a


def gather(ms, mt, st):
    v = pl.BlockSpec(memory_space=pltpu.VMEM)
    dma = pltpu.SemaphoreType.DMA
    return pl.pallas_call(
        gather_kernel,
        out_shape=(jax.ShapeDtypeStruct((2, 64, 32, 256), BF16), jax.ShapeDtypeStruct((64, 2, 1, 128), F32)),
        in_specs=[v, v, pl.BlockSpec(memory_space=pltpu.SMEM)], out_specs=(v, v),
        scratch_shapes=[pltpu.VMEM((2, 16, 256), BF16), pltpu.VMEM((1, 128), F32),
                        dma((4,)), dma((2,)), dma((9,)), dma((9,)), dma((63,)), dma((64,)), dma((64,)), dma((64,))],
        compiler_params=pltpu.CompilerParams(collective_id=0, has_side_effects=True),
    )(ms, mt, st)


def sweeps(*args):
    v = pl.BlockSpec(memory_space=pltpu.VMEM)
    return pl.pallas_call(
        kernel, out_shape=jax.ShapeDtypeStruct((128, 16, 128), F32), in_specs=[v] * 5, out_specs=v,
        scratch_shapes=[
            pltpu.VMEM((2048, 256), F32), pltpu.VMEM((2048, 256), F32),
            pltpu.VMEM((16384, 128), BF16), pltpu.VMEM((129, 16, 128), F32),
            pltpu.VMEM((256, 256), BF16), pltpu.VMEM((16, 256), BF16), pltpu.VMEM((256, 256), BF16)],
        compiler_params=pltpu.CompilerParams(vmem_limit_bytes=40 * 2**20),
    )(*args)


def untangle(src, out):
    for c in range(10):
        for half in range(2):
            m = src[half, :, c, :].T
            for k in range(16):
                out[k, c, 8 * half:8 * half + 8, :] = m[8 * k:8 * k + 8, :]


def solution(mesh):
    def local(x_init, w_in, w_out, mod_scale, mod_shift, step_size):
        buf, hs = gather(mod_scale, mod_shift, step_size)
        mine = sweeps(buf, hs, jnp.transpose(x_init, (2, 1, 0)), w_in, w_out.T)
        got = lax.all_to_all(mine, "time", 0, 0, tiled=True)
        v = pl.BlockSpec(memory_space=pltpu.VMEM)
        res = pl.pallas_call(untangle, out_shape=jax.ShapeDtypeStruct((16, 10, 16, 64), F32), in_specs=[v], out_specs=v)(got.reshape(2, 64, 16, 128))
        return jnp.transpose(res, (0, 3, 2, 1))

    return jax.shard_map(local, mesh=mesh, in_specs=(P("data"), P(), P(), P("time"), P("time"), P("time")), out_specs=P("time", "data"), check_vma=False)
```

```python
import functools

import jax
import jax.numpy as jnp
from jax import lax
from jax.experimental import pallas as pl
from jax.experimental.pallas import tpu as pltpu
from jax.sharding import PartitionSpec as P

MESH = pl.DeviceIdType.MESH
ROWS = 10
CUBE = 0.044715
ROOT = 0.7978845608028654
F32, BF16 = jnp.float32, jnp.bfloat16

def nn(a, b):
    return lax.dot_general(a, b, (((1,), (0,)), ((), ())), preferred_element_type=F32)

def act(y):
    q = y * ((2.0 * ROOT) + (8.0 * ROOT * CUBE) * (y * y))
    return (y + y * jnp.tanh(q)).astype(BF16)


def gather(ms, mt, st, buf, hs, own, hrow, sx, rx, sh, rh, sm, rm, sd, rd):
    me = lax.axis_index("time")
    core = me % 2
    x, y, z = (me // 2) % 4, (me // 8) % 4, me // 32
    a = x + core * (z - x)
    b = y
    c = z + core * (x - z)
    ka, kc = 1 + 15 * core, 16 - 15 * core

    def dev(da, db, dc):
        aa, bb, cc = (a + da) % 4, (b + db) % 4, (c + dc) % 4
        return 2 * (aa * ka + bb * 4 + cc * kc) + core

    def idx(da, db, dc):
        return ((c + dc) % 4) * 16 + ((b + db) % 4) * 4 + (a + da) % 4

    partner = me + 1 - 2 * core
    peers = [dev(1, 0, 0), dev(3, 0, 0), dev(2, 0, 0), dev(0, 1, 0), dev(0, 3, 0), dev(0, 2, 0),
             dev(0, 0, 1), dev(0, 0, 3), dev(0, 0, 2), partner]
    own[0] = ms[...]
    own[1] = mt[...]
    lane = lax.broadcasted_iota(jnp.int32, (1, 128), 1)
    row = jnp.zeros((1, 128), F32)
    for k in range(16):
        row = jnp.where(lane // 8 == k, st[k] * (0.5 / 256.0), row)
    hrow[...] = row

    barrier = pltpu.get_barrier_semaphore()
    for p in peers:
        pl.semaphore_signal(barrier, inc=1, device_id={"time": p}, device_id_type=MESH)
    pl.semaphore_wait(barrier, len(peers))

    def remote(src, dst, s, r, p):
        cp = pltpu.make_async_remote_copy(src_ref=src, dst_ref=dst, send_sem=s, recv_sem=r,
                                          device_id={"time": p}, device_id_type=MESH)
        cp.start()
        return cp

    mine = idx(0, 0, 0)
    sent = []
    half = pl.ds(pl.multiple_of(core * 16, 16), 16)
    other = pl.ds(pl.multiple_of(16 - core * 16, 16), 16)
    ex = remote(own.at[1 - core], buf.at[1 - core, idx_of(me, 1 - core), half], sx.at[0], rx.at[0], partner)
    hx = remote(hrow, hs.at[idx_of(me, 1 - core), core], sx.at[1], rx.at[1], partner)
    l1 = pltpu.make_async_copy(own.at[core], buf.at[core, mine, half], sx.at[2])
    l2 = pltpu.make_async_copy(hrow, hs.at[mine, core], sx.at[3])
    l1.start(); l2.start()
    ex.wait(); hx.wait(); l1.wait(); l2.wait()

    nsend = [0]
    def send(i, p):
        k = nsend[0]
        nsend[0] += 1
        sent.append(remote(buf.at[core, i], buf.at[core, i], sm.at[k], rm.at[i], p))
    def relay(i, k):
        sent.append(remote(buf.at[core, i], buf.at[core, i], sd.at[k], rd.at[i], partner))
    def arrive(i):
        pltpu.make_async_copy(buf.at[core, i], buf.at[core, i], rm.at[i]).wait()

    hn = [0]
    def hsend(ref, j, p):
        k = hn[0]
        hn[0] += 1
        sent.append(remote(ref, ref, sh.at[k], rh.at[k], p))
    def harrive(ref, k):
        pltpu.make_async_copy(ref, ref, rh.at[k]).wait()

    order = (0, 1, 3, 2)
    for d in order[1:]:
        send(mine, dev(d, 0, 0))
    hm = hs.at[mine]
    for d in order[1:]:
        hsend(hm, d, dev(d, 0, 0))
    relay(mine, 0)
    nrel = 1
    for da in order:
        i = idx(da, 0, 0)
        if da:
            arrive(i)
        for d in order[1:]:
            send(i, dev(0, d, 0))
        for d in (1, 3):
            send(i, dev(0, 0, d))
        if da:
            relay(i, nrel)
            nrel += 1
    for k, d in enumerate(order[1:]):
        harrive(hs.at[idx(-d % 4, 0, 0)], k)
    hb = hs.at[pl.ds(pl.multiple_of(c * 16 + b * 4, 4), 4)]
    for d in order[1:]:
        hsend(hb, d, dev(0, d, 0))
    for db in order[1:]:
        for da in order:
            i = idx(da, db, 0)
            arrive(i)
            for d in (1, 3):
                send(i, dev(0, 0, d))
            relay(i, nrel)
            nrel += 1
    for k, d in enumerate(order[1:]):
        harrive(hs.at[pl.ds(pl.multiple_of(c * 16 + ((b - d) % 4) * 4, 4), 4)], 3 + k)
    hc = hs.at[pl.ds(pl.multiple_of(c * 16, 16), 16)]
    for d in order[1:]:
        hsend(hc, d, dev(0, 0, d))
    n = 0
    for db in order:
        for da in order:
            for dc, step in ((3, 1), (1, 3)):
                i = idx(da, db, dc)
                arrive(i)
                if (n < 8) == (step == 1):
                    send(i, dev(0, 0, step))
                relay(i, nrel)
                nrel += 1
            n += 1
    for db in order:
        for da in order:
            i = idx(da, db, 2)
            arrive(i)
            relay(i, nrel)
            nrel += 1
    for k, d in enumerate(order[1:]):
        harrive(hs.at[pl.ds(pl.multiple_of(((c - d) % 4) * 16, 16), 16)], 6 + k)
    for i in range(64):
        pltpu.make_async_copy(buf.at[1 - core, i], buf.at[1 - core, i], rd.at[i]).wait()
    for cp in sent:
        cp.wait_send()


def idx_of(me, core):
    x, y, z = (me // 2) % 4, (me // 8) % 4, me // 32
    a, c = x + core * (z - x), z + core * (x - z)
    return c * 16 + y * 4 + a


def other(t):
    return (t % 4) * 16 + ((t // 4) % 4) * 4 + t // 16


def body(ms, mt, st, xt_, w_in, w_out, recv, offs, buf, hs, own, hrow, sf, bf, xg, db, wi, wo, tris, sb, tot, ob,
         sx, rx, sh, rh, sm, rm, sd, rd, sa, ra, so, ro, wz, yb, hb, eb):
    gather(ms, mt, st, buf, hs, own, hrow, sx, rx, sh, rh, sm, rm, sd, rd)
    db[128] = jnp.zeros((16, 128), F32)
    me = lax.axis_index("time")
    core = me % 2
    half, batch = me // 64, me % 64
    wi[...] = jnp.zeros_like(wi)
    wo[...] = jnp.zeros_like(wo)
    wi[0:10, :] = w_in[...]
    wo[0:10, :] = w_out[...]
    lane8 = lax.broadcasted_iota(jnp.int32, (8, 128), 1)
    pick = lax.broadcasted_iota(jnp.int32, (8, 64), 1) == batch
    xr = jnp.zeros((8, 128), F32)
    for ch in range(10):
        col = jnp.sum(jnp.where(pick, xt_[ch, pl.ds(pl.multiple_of(half * 8, 8), 8), :], 0.0), axis=1, keepdims=True)
        xr = jnp.where(lane8 == ch, col, xr)
    x0v = jnp.concatenate([xr] * 16, axis=0).T[0:16, :]
    xl = jnp.concatenate([jnp.concatenate([xr, jnp.zeros((8, 128), F32)], axis=0).astype(BF16), jnp.zeros((16, 128), BF16)], axis=1)
    ri = lax.broadcasted_iota(jnp.int32, (256, 256), 0) % 128
    ci = lax.broadcasted_iota(jnp.int32, (256, 256), 1)
    cm = ci % 128
    tri = jnp.where(((ri % 8) == (cm % 8)) & ((ci >= 128) | ((ri // 8) < (cm // 8))), 256.0, 0.0).astype(BF16)
    tris[...] = tri
    u = nn(xl[:, 0:128], wi[...])[:8]
    for k in range(8):
        wz[k] = jnp.zeros((128, 256), BF16)
        wz[k, 16 * k:16 * k + 16, :] = wi[0:16, :]
    wov = wo[...]

    def conv(t, _):
        r = pl.ds(pl.multiple_of(t * 32, 32), 32)
        sf[r, 0, :] = 0.5 + 0.5 * buf[0, t].astype(F32)
        bf[r, 0, :] = 0.5 * buf[1, other(t)].astype(F32)
        return 0
    lax.fori_loop(0, 64, conv, 0)

    def spread(ref, r0):
        return jnp.broadcast_to(ref[pl.ds(r0, 16)], (16, 8, 256)).reshape(128, 256)

    def hidden(g, tau, y):
        r0 = g * 256 + tau * 16
        return act(y * spread(sf, r0) + spread(bf, r0))

    def put(t, d):
        db[2 * t] = d[:, :128]
        db[2 * t + 1] = d[:, 128:]

    def nt(a, b):
        return lax.dot_general(a, b, (((1,), (1,)), ((), ())), preferred_element_type=F32)

    def project(t, h):
        put(t, nt(wov, h))

    def first(g, _):
        uu = jnp.concatenate([u] * 16, axis=0)
        project(lax.rem(8 * g + 63, 64), hb[...])
        for j in range(8):
            h = [hidden(g, 2 * j, uu), hidden(g, 2 * j + 1, uu)]
            h = jnp.concatenate(h, axis=0)
            if j < 7:
                project(8 * g + j, h)
            else:
                hb[...] = h
        return 0

    lane = lax.broadcasted_iota(jnp.int32, (16, 128), 1)
    zb = jnp.zeros((16, 128), BF16)

    def feed(g):
        rolled = None
        prs = []
        for i in range(16):
            t = g * 16 + i
            tile = g * 8 + i // 2
            tile = tile + core * (other(tile) - tile)
            d = db[t]
            here = pltpu.roll(d, 120, 1) if rolled is None else rolled
            rolled = pltpu.roll(db[t + 1], 120, 1)
            gr = (d + jnp.where(lane < 120, here, rolled)) * hs[tile, i % 2]
            hi = gr.astype(BF16)
            r1 = gr - hi.astype(F32)
            mid = r1.astype(BF16)
            lo = (r1 - mid.astype(F32)).astype(BF16)
            prs.append((hi, mid, lo))
        cat = lambda f: jnp.concatenate([f(p) for p in prs], axis=0)
        lhs = jnp.concatenate([cat(lambda p: p[0]), cat(lambda p: p[1])], axis=1)
        eb[...] = nn(lhs, tris[...]) + nn(cat(lambda p: p[2]), tris[0:128, :])

    def drain(carry):
        xs = []
        for i in range(16):
            xs.append(carry + eb[16 * i:16 * i + 16, :128])
            carry = carry + eb[16 * i:16 * i + 16, 128:]
        return xs, carry

    def store_x(g, xs):
        for q in range(2):
            xg[2 * g + q] = jnp.concatenate(xs[8 * q:8 * q + 8], axis=0).astype(BF16).T

    def lift(g, tau):
        return nn(xg[2 * g + tau // 8], wz[tau % 8])

    def drift(g, n):
        project(lax.rem(8 * g + 63, 64), hb[...])
        y = {k: yb[k] for k in range(3)}
        h = []
        for tau in range(16):
            if tau < 13:
                y[tau + 3] = lift(g, tau + 3)
            h += [hidden(g, tau, y[tau])]
            if tau >= 13:
                yb[tau - 13] = lift(n, tau - 13)
            if tau == 15:
                hb[...] = jnp.concatenate(h, axis=0)
            elif tau % 2:
                project(8 * g + tau // 2, jnp.concatenate(h, axis=0))
                h = []

    def later(i, carry):
        g = lax.rem(i, 8)
        n = lax.rem(i + 1, 8)
        carry = jnp.where(n == 0, x0v, carry)
        xs, carry = drain(carry)
        store_x(n, xs)
        feed(lax.rem(i + 2, 8))
        drift(g, n)
        return carry

    hb[...] = jnp.zeros_like(hb)
    lax.fori_loop(0, 8, first, 0)
    project(63, hb[...])
    feed(0)
    xs, carry = drain(x0v)
    store_x(0, xs)
    feed(1)
    for tau in range(3):
        yb[tau] = lift(0, tau)
    carry = lax.fori_loop(0, 16, later, carry)
    project(63, hb[...])

    def scan(g, carry):
        feed(g)
        xs, carry = drain(carry)
        store_x(g, xs)
        return carry
    lax.fori_loop(0, 8, scan, x0v)
    g0 = me % 8

    def collect(g):
        for i in range(16):
            sb[16 * g + i] = eb[16 * i:16 * i + 16, :128]
            tot[16 * g + i] = eb[16 * i:16 * i + 16, 128:]

    def ship(g):
        for i in range(16):
            q = 16 * g + i

            @pl.when(q != me)
            def _():
                bulk(q).start()

    def bulk(q):
        return pltpu.make_async_remote_copy(src_ref=sb.at[q, pl.ds(0, ROWS)], dst_ref=recv.at[me, pl.ds(0, ROWS)], send_sem=sa.at[q],
                                            recv_sem=ra.at[me], device_id={"time": q}, device_id_type=MESH)

    def last(drains, feeds):
        def run(i, _):
            g = lax.rem(g0 + i, 8)
            if drains:
                collect(lax.rem(g + 5, 8))
            if feeds:
                feed(lax.rem(g + 6, 8))
            drift(g, lax.rem(g + 1, 8))
            if drains:
                ship(lax.rem(g + 5, 8))
            return 0
        return run
    for tau in range(3):
        yb[tau] = lift(g0, tau)
    lax.fori_loop(0, 2, last(False, False), 0)
    last(False, True)(2, 0)
    lax.fori_loop(3, 8, last(True, True), 0)
    project(lax.rem(8 * g0 + 63, 64), hb[...])
    collect(lax.rem(g0 + 5, 8))
    feed(lax.rem(g0 + 6, 8))
    ship(lax.rem(g0 + 5, 8))
    collect(lax.rem(g0 + 6, 8))
    feed(lax.rem(g0 + 7, 8))
    ship(lax.rem(g0 + 6, 8))
    collect(lax.rem(g0 + 7, 8))

    diag = lane // 8 == lax.broadcasted_iota(jnp.int32, (16, 128), 0)

    def offsets(g, carry):
        for i in range(16):
            ob[16 * g + i] = jnp.sum(jnp.where(diag, carry, 0.0), axis=0, keepdims=True)
            carry = carry + tot[16 * g + i]
        return carry
    lax.fori_loop(0, 8, offsets, x0v)
    ship(lax.rem(g0 + 7, 8))

    def small(q):
        return pltpu.make_async_remote_copy(src_ref=ob.at[q], dst_ref=offs.at[me], send_sem=so.at[q],
                                            recv_sem=ro.at[me], device_id={"time": q}, device_id_type=MESH)

    def post(k, _):
        small(lax.rem(me + k, 128)).start()
        return 0
    lax.fori_loop(1, 128, post, 0)
    recv[me] = sb[me]
    offs[me] = ob[me]

    def settle(k, _):
        q = lax.rem(me + k, 128)
        bulk(q).wait_send()
        small(q).wait_send()
        pltpu.make_async_copy(recv.at[q, pl.ds(0, ROWS)], recv.at[q, pl.ds(0, ROWS)], ra.at[q]).wait()
        pltpu.make_async_copy(offs.at[q], offs.at[q], ro.at[q]).wait()
        return 0
    lax.fori_loop(1, 128, settle, 0)


def sweeps(*args):
    v = pl.BlockSpec(memory_space=pltpu.VMEM)
    dma = pltpu.SemaphoreType.DMA
    return pl.pallas_call(
        body,
        out_shape=(jax.ShapeDtypeStruct((128, 16, 128), F32), jax.ShapeDtypeStruct((128, 1, 128), F32)),
        in_specs=[v, v, pl.BlockSpec(memory_space=pltpu.SMEM), v, v, v], out_specs=(v, v),
        scratch_shapes=[
            pltpu.VMEM((2, 64, 32, 256), BF16), pltpu.VMEM((64, 2, 1, 128), F32),
            pltpu.VMEM((2, 16, 256), BF16), pltpu.VMEM((1, 128), F32),
            pltpu.VMEM((2048, 1, 256), F32), pltpu.VMEM((2048, 1, 256), F32),
            pltpu.VMEM((16, 128, 128), BF16), pltpu.VMEM((129, 16, 128), F32),
            pltpu.VMEM((128, 256), BF16), pltpu.VMEM((16, 256), BF16), pltpu.VMEM((256, 256), BF16),
            pltpu.VMEM((128, 16, 128), F32), pltpu.VMEM((128, 16, 128), F32), pltpu.VMEM((128, 1, 128), F32),
            dma((4,)), dma((2,)), dma((9,)), dma((9,)), dma((63,)), dma((64,)), dma((64,)), dma((64,)),
            dma((128,)), dma((128,)), dma((128,)), dma((128,)),
            pltpu.VMEM((8, 128, 256), BF16), pltpu.VMEM((3, 128, 256), F32), pltpu.VMEM((256, 256), BF16), pltpu.VMEM((256, 256), F32)],
        compiler_params=pltpu.CompilerParams(vmem_limit_bytes=40 * 2**20, collective_id=0, has_side_effects=True),
    )(*args)


def untangle(src, off, out):
    for half in range(2):
        base = off[64 * half:64 * half + 64, :].T
        for c in range(10):
            m = src[half, :, c, :].T
            for k in range(16):
                out[k, c, 8 * half:8 * half + 8, :] = m[8 * k:8 * k + 8, :] + base[8 * c:8 * c + 8, :]


def solution(mesh):
    def local(x_init, w_in, w_out, mod_scale, mod_shift, step_size):
        got, off = sweeps(mod_scale, mod_shift, step_size, jnp.transpose(x_init, (2, 1, 0)), w_in, w_out.T)
        v = pl.BlockSpec(memory_space=pltpu.VMEM)
        res = pl.pallas_call(untangle, out_shape=jax.ShapeDtypeStruct((16, 10, 16, 64), F32), in_specs=[v, v], out_specs=v)(
            got.reshape(2, 64, 16, 128), off.reshape(128, 128))
        return jnp.transpose(res, (0, 3, 2, 1))

    return jax.shard_map(local, mesh=mesh, in_specs=(P("data"), P(), P(), P("time"), P("time"), P("time")), out_specs=P("time", "data"), check_vma=False)
```

```python
import functools

import jax
import jax.numpy as jnp
from jax import lax
from jax.experimental import pallas as pl
from jax.experimental.pallas import tpu as pltpu
from jax.sharding import PartitionSpec as P

MESH = pl.DeviceIdType.MESH
ROWS = 10
CUBE = 0.044715
ROOT = 0.7978845608028654
F32, BF16 = jnp.float32, jnp.bfloat16

def nn(a, b):
    return lax.dot_general(a, b, (((1,), (0,)), ((), ())), preferred_element_type=F32)

def act(y):
    q = y * ((2.0 * ROOT) + (8.0 * ROOT * CUBE) * (y * y))
    return (y + y * jnp.tanh(q)).astype(BF16)


def coords(me):
    return (me // 2) % 4, (me // 8) % 4, me // 32


def gather(ms, mt, st, buf, hs, sl, ss, sh, rab, rc, rf, rd, rh):
    me = lax.axis_index("time")
    core = me % 2
    x, y, z = coords(me)
    a = x + core * (z - x)
    b = y
    c = z + core * (x - z)
    ka, kc = 1 + 15 * core, 16 - 15 * core
    base = core * 64

    def dev(da, db, dc):
        aa, bb, cc = (a + da) % 4, (b + db) % 4, (c + dc) % 4
        return 2 * (aa * ka + bb * 4 + cc * kc) + core

    def group(db, dc):
        return pl.ds(pl.multiple_of(base + ((c + dc) % 4) * 16 + ((b + db) % 4) * 4, 4), 4)

    partner = me + 1 - 2 * core
    mine = base + c * 16 + b * 4 + a
    plane = [(da, db) for db in (0, 1, 3, 2) for da in (0, 1, 3, 2) if da or db]
    peers = [dev(da, db, 0) for da, db in plane] + [dev(0, 0, 1), dev(0, 0, 3), dev(0, 0, 2), partner]

    barrier = pltpu.get_barrier_semaphore()
    for p in peers:
        pl.semaphore_signal(barrier, inc=1, device_id={"time": p}, device_id_type=MESH)
    loads = [pltpu.make_async_copy(ms, buf.at[mine, 0], sl.at[0]), pltpu.make_async_copy(mt, buf.at[mine, 1], sl.at[1])]
    for cp in loads:
        cp.start()
    lane = lax.broadcasted_iota(jnp.int32, (1, 128), 1)
    row = jnp.zeros((1, 128), F32)
    for k in range(16):
        row = jnp.where(lane // 8 == k, st[k] * (0.5 / 256.0), row)
    hs[mine] = row
    for cp in loads:
        cp.wait()
    pl.semaphore_wait(barrier, len(peers))

    def send(ref, s, r, p):
        pltpu.make_async_remote_copy(src_ref=ref, dst_ref=ref, send_sem=s, recv_sem=r,
                                     device_id={"time": p}, device_id_type=MESH).start()

    def arrive(ref, r):
        pltpu.make_async_copy(ref, ref, r).wait()

    for da, db in plane:
        send(buf.at[mine], ss, rab.at[db], dev(da, db, 0))
    for da, db in plane:
        send(hs.at[mine], sh, rh.at[0], dev(da, db, 0))
    order = (0, 1, 3, 2)
    for db in order:
        ref = buf.at[group(4 - db, 0)]
        if db:
            arrive(ref, rab.at[db])
        else:
            arrive(buf.at[pl.ds(0, 3)], rab.at[0])
        send(ref, ss, rc.at[0, db], dev(0, 0, 1))
        send(ref, ss, rc.at[1, db], dev(0, 0, 3))
        send(ref, ss, rd.at[0], partner)
    arrive(hs.at[pl.ds(0, 15)], rh.at[0])
    rows = hs.at[pl.ds(pl.multiple_of(base + c * 16, 16), 16)]
    for d in (1, 3, 2):
        send(rows, sh, rh.at[1], dev(0, 0, d))
    for n, db in enumerate(order):
        up = buf.at[group(4 - db, 3)]
        arrive(up, rc.at[0, db])
        if n < 2:
            send(up, ss, rf.at[db], dev(0, 0, 1))
        send(up, ss, rd.at[1], partner)
        down = buf.at[group(4 - db, 1)]
        arrive(down, rc.at[1, db])
        if n >= 2:
            send(down, ss, rf.at[db], dev(0, 0, 3))
        send(down, ss, rd.at[2], partner)
    arrive(hs.at[pl.ds(0, 48)], rh.at[1])
    send(hs.at[pl.ds(pl.multiple_of(base, 64), 64)], sh, rh.at[2], partner)
    for db in order:
        far = buf.at[group(4 - db, 2)]
        arrive(far, rf.at[db])
        send(far, ss, rd.at[3], partner)
    for k in range(4):
        arrive(buf.at[pl.ds(0, 16)], rd.at[k])
    arrive(hs.at[pl.ds(0, 64)], rh.at[2])
    arrive(buf.at[pl.ds(0, 127)], ss)
    arrive(hs.at[pl.ds(0, 127)], sh)


def other(t):
    return (t % 4) * 16 + ((t // 4) % 4) * 4 + t // 16


def body(ms, mt, st, xh, wih, woh, recv, offs, buf, hs, xt_, w_in, w_out, sf, bf, xg, db, wi, wo, tris, sb, tot, ob,
         sl, ss, sh, rab, rc, rf, rd, rh, sa, wz, yb, hb, eb):
    early = [pltpu.make_async_copy(*pair, sl.at[2 + k]) for k, pair in enumerate(((xh, xt_), (wih, w_in), (woh, w_out)))]
    for cp in early:
        cp.start()
    gather(ms, mt, st, buf, hs, sl, ss, sh, rab, rc, rf, rd, rh)
    for cp in early:
        cp.wait()
    db[128] = jnp.zeros((16, 128), F32)
    me = lax.axis_index("time")
    core = me % 2
    half, batch = me // 64, me % 64
    wi[...] = jnp.zeros_like(wi)
    wo[...] = jnp.zeros_like(wo)
    wi[0:10, :] = w_in[...]
    wo[0:10, :] = w_out[...]
    lane8 = lax.broadcasted_iota(jnp.int32, (8, 128), 1)
    pick = lax.broadcasted_iota(jnp.int32, (8, 64), 1) == batch
    xr = jnp.zeros((8, 128), F32)
    for ch in range(10):
        col = jnp.sum(jnp.where(pick, xt_[ch, pl.ds(pl.multiple_of(half * 8, 8), 8), :], 0.0), axis=1, keepdims=True)
        xr = jnp.where(lane8 == ch, col, xr)
    x0v = jnp.concatenate([xr] * 16, axis=0).T[0:16, :]
    xl = jnp.concatenate([jnp.concatenate([xr, jnp.zeros((8, 128), F32)], axis=0).astype(BF16), jnp.zeros((16, 128), BF16)], axis=1)
    ri = lax.broadcasted_iota(jnp.int32, (256, 256), 0) % 128
    ci = lax.broadcasted_iota(jnp.int32, (256, 256), 1)
    cm = ci % 128
    tri = jnp.where(((ri % 8) == (cm % 8)) & ((ci >= 128) | ((ri // 8) < (cm // 8))), 256.0, 0.0).astype(BF16)
    tris[...] = tri
    u = nn(xl[:, 0:128], wi[...])[:8]
    for k in range(8):
        wz[k] = jnp.zeros((128, 256), BF16)
        wz[k, 16 * k:16 * k + 16, :] = wi[0:16, :]
    wov = wo[...]

    def conv(t, _):
        for q, n in ((0, t), (1, 64 + other(t))):
            r = pl.ds(t * 32 + 16 * q, 16)
            sf[r, 0, :] = 0.5 + 0.5 * buf[n, 0].astype(F32)
            bf[r, 0, :] = 0.5 * buf[n, 1].astype(F32)
        return 0
    lax.fori_loop(0, 64, conv, 0)

    def spread(ref, r0):
        return jnp.broadcast_to(ref[pl.ds(r0, 16)], (16, 8, 256)).reshape(128, 256)

    def hidden(g, tau, y):
        r0 = g * 256 + tau * 16
        return act(y * spread(sf, r0) + spread(bf, r0))

    def put(t, d):
        db[2 * t] = d[:, :128]
        db[2 * t + 1] = d[:, 128:]

    def nt(a, b):
        return lax.dot_general(a, b, (((1,), (1,)), ((), ())), preferred_element_type=F32)

    def project(t, h):
        put(t, nt(wov, h))

    def first(g, _):
        uu = jnp.concatenate([u] * 16, axis=0)
        project(lax.rem(8 * g + 63, 64), hb[...])
        for j in range(8):
            h = [hidden(g, 2 * j, uu), hidden(g, 2 * j + 1, uu)]
            h = jnp.concatenate(h, axis=0)
            if j < 7:
                project(8 * g + j, h)
            else:
                hb[...] = h
        return 0

    lane = lax.broadcasted_iota(jnp.int32, (16, 128), 1)
    zb = jnp.zeros((16, 128), BF16)

    def feed(g):
        rolled = None
        prs = []
        for i in range(16):
            t = g * 16 + i
            tile = g * 8 + i // 2
            tile = 64 + other(tile) if i % 2 else tile
            d = db[t]
            here = pltpu.roll(d, 120, 1) if rolled is None else rolled
            rolled = pltpu.roll(db[t + 1], 120, 1)
            gr = (d + jnp.where(lane < 120, here, rolled)) * hs[tile]
            hi = gr.astype(BF16)
            r1 = gr - hi.astype(F32)
            mid = r1.astype(BF16)
            lo = (r1 - mid.astype(F32)).astype(BF16)
            prs.append((hi, mid, lo))
        cat = lambda f: jnp.concatenate([f(p) for p in prs], axis=0)
        lhs = jnp.concatenate([cat(lambda p: p[0]), cat(lambda p: p[1])], axis=1)
        eb[...] = nn(lhs, tris[...]) + nn(cat(lambda p: p[2]), tris[0:128, :])

    def drain(carry):
        xs = []
        for i in range(16):
            xs.append(carry + eb[16 * i:16 * i + 16, :128])
            carry = carry + eb[16 * i:16 * i + 16, 128:]
        return xs, carry

    def store_x(g, xs):
        for q in range(2):
            xg[2 * g + q] = jnp.concatenate(xs[8 * q:8 * q + 8], axis=0).astype(BF16).T

    def lift(g, tau):
        return nn(xg[2 * g + tau // 8], wz[tau % 8])

    def drift(g, n):
        project(lax.rem(8 * g + 63, 64), hb[...])
        y = {k: yb[k] for k in range(3)}
        h = []
        for tau in range(16):
            if tau < 13:
                y[tau + 3] = lift(g, tau + 3)
            h += [hidden(g, tau, y[tau])]
            if tau >= 13:
                yb[tau - 13] = lift(n, tau - 13)
            if tau == 15:
                hb[...] = jnp.concatenate(h, axis=0)
            elif tau % 2:
                project(8 * g + tau // 2, jnp.concatenate(h, axis=0))
                h = []

    def later(i, carry):
        g = lax.rem(i, 8)
        n = lax.rem(i + 1, 8)
        carry = jnp.where(n == 0, x0v, carry)
        xs, carry = drain(carry)
        store_x(n, xs)
        feed(lax.rem(i + 2, 8))
        drift(g, n)
        return carry

    hb[...] = jnp.zeros_like(hb)
    lax.fori_loop(0, 8, first, 0)
    project(63, hb[...])
    feed(0)
    xs, carry = drain(x0v)
    store_x(0, xs)
    feed(1)
    for tau in range(3):
        yb[tau] = lift(0, tau)
    carry = lax.fori_loop(0, 16, later, carry)
    project(63, hb[...])

    def scan(g, carry):
        feed(g)
        xs, carry = drain(carry)
        store_x(g, xs)
        return carry
    lax.fori_loop(0, 8, scan, x0v)
    g0 = me % 8

    def collect(g):
        for i in range(16):
            sb[16 * g + i] = eb[16 * i:16 * i + 16, :128]
            tot[16 * g + i] = eb[16 * i:16 * i + 16, 128:]

    def ship(g):
        for i in range(16):
            q = 16 * g + i

            @pl.when(q != me)
            def _():
                bulk(q).start()

    def bulk(q):
        return pltpu.make_async_remote_copy(src_ref=sb.at[q, pl.ds(0, ROWS)], dst_ref=recv.at[me, pl.ds(0, ROWS)], send_sem=sa.at[0],
                                            recv_sem=sa.at[1], device_id={"time": q}, device_id_type=MESH)

    def last(drains, feeds):
        def run(i, _):
            g = lax.rem(g0 + i, 8)
            if drains:
                collect(lax.rem(g + 5, 8))
            if feeds:
                feed(lax.rem(g + 6, 8))
            drift(g, lax.rem(g + 1, 8))
            if drains:
                ship(lax.rem(g + 5, 8))
            return 0
        return run
    for tau in range(3):
        yb[tau] = lift(g0, tau)
    lax.fori_loop(0, 2, last(False, False), 0)
    last(False, True)(2, 0)
    lax.fori_loop(3, 8, last(True, True), 0)
    project(lax.rem(8 * g0 + 63, 64), hb[...])
    collect(lax.rem(g0 + 5, 8))
    feed(lax.rem(g0 + 6, 8))
    ship(lax.rem(g0 + 5, 8))
    collect(lax.rem(g0 + 6, 8))
    feed(lax.rem(g0 + 7, 8))
    ship(lax.rem(g0 + 6, 8))
    collect(lax.rem(g0 + 7, 8))

    diag = lane // 8 == lax.broadcasted_iota(jnp.int32, (16, 128), 0)

    def offsets(g, carry):
        for i in range(16):
            ob[16 * g + i] = jnp.sum(jnp.where(diag, carry, 0.0), axis=0, keepdims=True)
            carry = carry + tot[16 * g + i]
        return carry
    lax.fori_loop(0, 8, offsets, x0v)
    ship(lax.rem(g0 + 7, 8))

    def small(q):
        return pltpu.make_async_remote_copy(src_ref=ob.at[q], dst_ref=offs.at[me], send_sem=sa.at[2],
                                            recv_sem=sa.at[3], device_id={"time": q}, device_id_type=MESH)

    def post(k, _):
        small(lax.rem(me + k, 128)).start()
        return 0
    lax.fori_loop(1, 128, post, 0)
    recv[me] = sb[me]
    offs[me] = ob[me]

    for k, ref in enumerate((sb.at[pl.ds(0, 127), pl.ds(0, ROWS)], recv.at[pl.ds(0, 127), pl.ds(0, ROWS)],
                             ob.at[pl.ds(0, 127)], offs.at[pl.ds(0, 127)])):
        pltpu.make_async_copy(ref, ref, sa.at[k]).wait()


def sweeps(*args):
    v = pl.BlockSpec(memory_space=pltpu.VMEM)
    h = pl.BlockSpec(memory_space=pltpu.HBM)
    dma = pltpu.SemaphoreType.DMA
    return pl.pallas_call(
        body,
        out_shape=(jax.ShapeDtypeStruct((128, 16, 128), F32), jax.ShapeDtypeStruct((128, 1, 128), F32)),
        in_specs=[h, h, pl.BlockSpec(memory_space=pltpu.SMEM), h, h, h], out_specs=(v, v),
        scratch_shapes=[
            pltpu.VMEM((128, 2, 16, 256), BF16), pltpu.VMEM((128, 1, 128), F32),
            pltpu.VMEM((10, 16, 64), F32), pltpu.VMEM((10, 256), BF16), pltpu.VMEM((10, 256), BF16),
            pltpu.VMEM((2048, 1, 256), F32), pltpu.VMEM((2048, 1, 256), F32),
            pltpu.VMEM((16, 128, 128), BF16), pltpu.VMEM((129, 16, 128), F32),
            pltpu.VMEM((128, 256), BF16), pltpu.VMEM((16, 256), BF16), pltpu.VMEM((256, 256), BF16),
            pltpu.VMEM((128, 16, 128), F32), pltpu.VMEM((128, 16, 128), F32), pltpu.VMEM((128, 1, 128), F32),
            dma((5,)), dma, dma, dma((4,)), dma((2, 4)), dma((4,)), dma((4,)), dma((3,)), dma((4,)),
            pltpu.VMEM((8, 128, 256), BF16), pltpu.VMEM((3, 128, 256), F32), pltpu.VMEM((256, 256), BF16), pltpu.VMEM((256, 256), F32)],
        compiler_params=pltpu.CompilerParams(vmem_limit_bytes=58 * 2**20, collective_id=0, has_side_effects=True),
    )(*args)


def untangle(src, off, out):
    for half in range(2):
        base = off[64 * half:64 * half + 64, :].T
        for c in range(10):
            m = src[half, :, c, :].T
            for k in range(16):
                out[k, c, 8 * half:8 * half + 8, :] = m[8 * k:8 * k + 8, :] + base[8 * c:8 * c + 8, :]


def solution(mesh):
    def local(x_init, w_in, w_out, mod_scale, mod_shift, step_size):
        got, off = sweeps(mod_scale, mod_shift, step_size, jnp.transpose(x_init, (2, 1, 0)), w_in, w_out.T)
        v = pl.BlockSpec(memory_space=pltpu.VMEM)
        res = pl.pallas_call(untangle, out_shape=jax.ShapeDtypeStruct((16, 10, 16, 64), F32), in_specs=[v, v], out_specs=v)(
            got.reshape(2, 64, 16, 128), off.reshape(128, 128))
        return jnp.transpose(res, (0, 3, 2, 1))

    return jax.shard_map(local, mesh=mesh, in_specs=(P("data"), P(), P(), P("time"), P("time"), P("time")), out_specs=P("time", "data"), check_vma=False)
```

```python
import functools

import jax
import jax.numpy as jnp
from jax import lax
from jax.experimental import pallas as pl
from jax.experimental.pallas import tpu as pltpu
from jax.sharding import PartitionSpec as P

MESH = pl.DeviceIdType.MESH
ROWS = 10
FEED = 9
CUBE = 0.044715
ROOT = 0.7978845608028654
F32, BF16 = jnp.float32, jnp.bfloat16

def nn(a, b):
    return lax.dot_general(a, b, (((1,), (0,)), ((), ())), preferred_element_type=F32)

def act(y):
    q = y * ((2.0 * ROOT) + (8.0 * ROOT * CUBE) * (y * y))
    return (y + y * jnp.tanh(q)).astype(BF16)


def coords(me):
    return (me // 2) % 4, (me // 8) % 4, me // 32


def gather(ms, mt, st, buf, hs, sl, ss, sh, rab, rc, rf, rd, rh, ready, work):
    me = lax.axis_index("time")
    core = me % 2
    x, y, z = coords(me)
    a = x + core * (z - x)
    b = y
    c = z + core * (x - z)
    ka, kc = 1 + 15 * core, 16 - 15 * core
    base = core * 64

    def dev(da, db, dc):
        aa, bb, cc = (a + da) % 4, (b + db) % 4, (c + dc) % 4
        return 2 * (aa * ka + bb * 4 + cc * kc) + core

    def group(db, dc):
        return pl.ds(pl.multiple_of(base + ((c + dc) % 4) * 16 + ((b + db) % 4) * 4, 4), 4)

    partner = me + 1 - 2 * core
    mine = base + c * 16 + b * 4 + a
    plane = [(da, db) for db in (0, 1, 3, 2) for da in (0, 1, 3, 2) if da or db]
    peers = [dev(da, db, 0) for da, db in plane] + [dev(0, 0, 1), dev(0, 0, 3), dev(0, 0, 2), partner]

    barrier = pltpu.get_barrier_semaphore()
    for p in peers:
        pl.semaphore_signal(barrier, inc=1, device_id={"time": p}, device_id_type=MESH)
    loads = [pltpu.make_async_copy(ms, buf.at[mine, 0], sl.at[0]), pltpu.make_async_copy(mt, buf.at[mine, 1], sl.at[1])]
    for cp in loads:
        cp.start()
    lane = lax.broadcasted_iota(jnp.int32, (1, 128), 1)
    row = jnp.zeros((1, 128), F32)
    for k in range(16):
        row = jnp.where(lane // 8 == k, st[k] * (0.5 / 256.0), row)
    hs[mine] = row
    for cp in loads:
        cp.wait()
    pl.semaphore_wait(barrier, len(peers))

    def send(ref, s, r, p):
        pltpu.make_async_remote_copy(src_ref=ref, dst_ref=ref, send_sem=s, recv_sem=r,
                                     device_id={"time": p}, device_id_type=MESH).start()

    def arrive(ref, r):
        pltpu.make_async_copy(ref, ref, r).wait()

    for da, db in plane:
        send(buf.at[mine], ss, rab.at[db], dev(da, db, 0))
    for da, db in plane:
        send(hs.at[mine], sh, rh.at[0], dev(da, db, 0))
    ready()
    order = (0, 1, 3, 2)
    for db in order:
        ref = buf.at[group(4 - db, 0)]
        if db:
            arrive(ref, rab.at[db])
        else:
            arrive(buf.at[pl.ds(0, 3)], rab.at[0])
        send(ref, ss, rc.at[0, db], dev(0, 0, 1))
        send(ref, ss, rc.at[1, db], dev(0, 0, 3))
        send(ref, ss, rd.at[0], partner)
    arrive(hs.at[pl.ds(0, 15)], rh.at[0])
    rows = hs.at[pl.ds(pl.multiple_of(base + c * 16, 16), 16)]
    for d in (1, 3, 2):
        send(rows, sh, rh.at[1], dev(0, 0, d))

    def run(db, dc):
        return base + ((c + dc) % 4) * 16 + ((b + db) % 4) * 4

    pc = x + core * (z - x)
    pbase = 64 - base

    def prun(k, dc):
        return pbase + ((pc + dc) % 4) * 16 + 4 * k

    work([run(k, 0) for k in range(4)])
    arrive(buf.at[pl.ds(0, 16)], rd.at[0])
    work([prun(k, 0) for k in range(4)])
    for n, db in enumerate(order):
        up = buf.at[group(4 - db, 3)]
        arrive(up, rc.at[0, db])
        if n < 2:
            send(up, ss, rf.at[db], dev(0, 0, 1))
        send(up, ss, rd.at[1], partner)
        down = buf.at[group(4 - db, 1)]
        arrive(down, rc.at[1, db])
        if n >= 2:
            send(down, ss, rf.at[db], dev(0, 0, 3))
        send(down, ss, rd.at[2], partner)
        if n < 3:
            work([run(4 - db, 3), run(4 - db, 1)])
    arrive(hs.at[pl.ds(0, 48)], rh.at[1])
    send(hs.at[pl.ds(pl.multiple_of(base, 64), 64)], sh, rh.at[2], partner)
    for db in order:
        far = buf.at[group(4 - db, 2)]
        arrive(far, rf.at[db])
        send(far, ss, rd.at[3], partner)
    work([run(4 - order[3], 3), run(4 - order[3], 1)])
    arrive(buf.at[pl.ds(0, 16)], rd.at[1])
    work([prun(k, 3) for k in range(4)])
    arrive(buf.at[pl.ds(0, 16)], rd.at[2])
    work([prun(k, 1) for k in range(4)])
    work([run(k, 2) for k in range(4)])
    arrive(buf.at[pl.ds(0, 16)], rd.at[3])
    work([prun(k, 2) for k in range(4)])
    arrive(hs.at[pl.ds(0, 64)], rh.at[2])
    arrive(buf.at[pl.ds(0, 127)], ss)
    arrive(hs.at[pl.ds(0, 127)], sh)


def other(t):
    return (t % 4) * 16 + ((t // 4) % 4) * 4 + t // 16


def body(ms, mt, st, xh, wih, woh, recv, offs, buf, hs, xt_, w_in, w_out, sf, bf, xg, db, wi, wo, tris, sb, tot, ob,
         sl, ss, sh, rab, rc, rf, rd, rh, sa, wz, yb, hb, eb, ub, x0s):
    early = [pltpu.make_async_copy(*pair, sl.at[2 + k]) for k, pair in enumerate(((xh, xt_), (wih, w_in), (woh, w_out)))]
    for cp in early:
        cp.start()
    db[128] = jnp.zeros((16, 128), F32)
    me = lax.axis_index("time")
    core = me % 2
    half, batch = me // 64, me % 64
    def prepare():
        wi[...] = jnp.zeros_like(wi)
        wo[...] = jnp.zeros_like(wo)
        wi[0:10, :] = w_in[...]
        wo[0:10, :] = w_out[...]
        lane8 = lax.broadcasted_iota(jnp.int32, (8, 128), 1)
        pick = lax.broadcasted_iota(jnp.int32, (8, 64), 1) == batch
        xr = jnp.zeros((8, 128), F32)
        for ch in range(10):
            col = jnp.sum(jnp.where(pick, xt_[ch, pl.ds(pl.multiple_of(half * 8, 8), 8), :], 0.0), axis=1, keepdims=True)
            xr = jnp.where(lane8 == ch, col, xr)
        x0v = jnp.concatenate([xr] * 16, axis=0).T[0:16, :]
        xl = jnp.concatenate([jnp.concatenate([xr, jnp.zeros((8, 128), F32)], axis=0).astype(BF16), jnp.zeros((16, 128), BF16)], axis=1)
        ri = lax.broadcasted_iota(jnp.int32, (256, 256), 0) % 128
        ci = lax.broadcasted_iota(jnp.int32, (256, 256), 1)
        cm = ci % 128
        tri = jnp.where(((ri % 8) == (cm % 8)) & ((ci >= 128) | ((ri // 8) < (cm // 8))), 256.0, 0.0).astype(BF16)
        tris[...] = tri
        u = nn(xl[:, 0:128], wi[...])[:8]
        for k in range(8):
            wz[k] = jnp.zeros((128, 256), BF16)
            wz[k, 16 * k:16 * k + 16, :] = wi[0:16, :]
        x0s[...] = x0v
        ub[...] = jnp.concatenate([u] * 16, axis=0)

    def spread(ref, r0):
        return jnp.broadcast_to(ref[pl.ds(r0, 16)], (16, 8, 256)).reshape(128, 256)

    def hidden(g, tau, y):
        r0 = g * 256 + tau * 16
        return act(y * spread(sf, r0) + spread(bf, r0))

    def put(t, d):
        db[2 * t] = d[:, :128]
        db[2 * t + 1] = d[:, 128:]

    def nt(a, b):
        return lax.dot_general(a, b, (((1,), (1,)), ((), ())), preferred_element_type=F32)

    def project(t, h):
        put(t, nt(wov, h))

    def ready():
        for cp in early:
            cp.wait()
        prepare()

    def work(runs):
        uu = ub[...]
        h = []
        blocks = [(n + k, k) for n in runs for k in range(4)]
        for q, (n, _) in enumerate(blocks):
            tree = n // 64
            idx = n - 64 * tree
            t = 2 * (idx + tree * (other(idx) - idx)) + tree
            r = pl.ds(t * 16, 16)
            sf[r, 0, :] = 0.5 + 0.5 * buf[n, 0].astype(F32)
            bf[r, 0, :] = 0.5 * buf[n, 1].astype(F32)
            h.append(act(uu * spread(sf, t * 16) + spread(bf, t * 16)))
            if q % 2:
                d = nt(wo[...], jnp.concatenate(h, axis=0))
                db[tp] = d[:, :128]
                db[t] = d[:, 128:]
                h = []
            tp = t

    lane = lax.broadcasted_iota(jnp.int32, (16, 128), 1)
    zb = jnp.zeros((16, 128), BF16)

    def feed(g):
        rolled = None
        prs = []
        for i in range(16):
            t = g * 16 + i
            tile = g * 8 + i // 2
            tile = 64 + other(tile) if i % 2 else tile
            d = db[t]
            here = pltpu.roll(d, 120, 1) if rolled is None else rolled
            rolled = pltpu.roll(db[t + 1], 120, 1)
            gr = (d + jnp.where(lane < 120, here, rolled)) * hs[tile]
            hi = gr.astype(BF16)
            r1 = gr - hi.astype(F32)
            mid = r1.astype(BF16)
            lo = (r1 - mid.astype(F32)).astype(BF16)
            prs.append((hi, mid, lo))
        cat = lambda f: jnp.concatenate([f(p) for p in prs], axis=0)
        lhs = jnp.concatenate([cat(lambda p: p[0]), cat(lambda p: p[1])], axis=1)
        eb[...] = nn(lhs, tris[...]) + nn(cat(lambda p: p[2]), tris[0:128, :])

    def drain(carry):
        xs = []
        for i in range(16):
            xs.append(carry + eb[16 * i:16 * i + 16, :128])
            carry = carry + eb[16 * i:16 * i + 16, 128:]
        return xs, carry

    def store_x(g, xs):
        for q in range(2):
            xg[2 * g + q] = jnp.concatenate(xs[8 * q:8 * q + 8], axis=0).astype(BF16).T

    def lift(g, tau):
        return nn(xg[2 * g + tau // 8], wz[tau % 8])

    def drift(g, n, hooks={}):
        project(lax.rem(8 * g + 63, 64), hb[...])
        y = {k: yb[k] for k in range(3)}
        h = []
        for tau in range(16):
            if tau < 13:
                y[tau + 3] = lift(g, tau + 3)
            if 11 <= tau < 14:
                yb[tau - 11] = lift(n, tau - 11)
            h += [hidden(g, tau, y[tau])]
            if tau in hooks:
                hooks[tau]()
            if tau == 15:
                hb[...] = jnp.concatenate(h, axis=0)
            elif tau % 2:
                project(8 * g + tau // 2, jnp.concatenate(h, axis=0))
                h = []

    def later(i, carry):
        g = lax.rem(i, 8)
        n = lax.rem(i + 1, 8)
        carry = jnp.where(n == 0, x0v, carry)
        xs, carry = drain(carry)
        store_x(n, xs)
        feed(lax.rem(i + 2, 8))
        drift(g, n)
        return carry

    gather(ms, mt, st, buf, hs, sl, ss, sh, rab, rc, rf, rd, rh, ready, work)
    x0v = x0s[...]
    wov = wo[...]
    hb[...] = jnp.zeros_like(hb)
    feed(0)
    xs, carry = drain(x0v)
    store_x(0, xs)
    feed(1)
    for tau in range(3):
        yb[tau] = lift(0, tau)
    carry = lax.fori_loop(0, 16, later, carry)
    project(63, hb[...])

    def scan(g, carry):
        feed(g)
        xs, carry = drain(carry)
        store_x(g, xs)
        return carry
    lax.fori_loop(0, 8, scan, x0v)
    g0 = me % 8

    def collect(g):
        for i in range(16):
            sb[16 * g + i] = eb[16 * i:16 * i + 16, :128]
            tot[16 * g + i] = eb[16 * i:16 * i + 16, 128:]

    def ship(g):
        for i in range(16):
            q = 16 * g + i

            @pl.when(q != me)
            def _():
                bulk(q).start()

    def bulk(q):
        return pltpu.make_async_remote_copy(src_ref=sb.at[q, pl.ds(0, ROWS)], dst_ref=recv.at[me, pl.ds(0, ROWS)], send_sem=sa.at[0],
                                            recv_sem=sa.at[1], device_id={"time": q}, device_id_type=MESH)

    def last(feeds, ships):
        def run(i, _):
            g = lax.rem(g0 + i, 8)
            hooks = {}
            if ships:
                hooks[2] = lambda: ship(lax.rem(g + 6, 8))
            if feeds:
                hooks[FEED] = lambda: feed(lax.rem(g + 7, 8))
            drift(g, lax.rem(g + 1, 8), hooks)
            if feeds:
                collect(lax.rem(g + 7, 8))
            return 0
        return run
    for tau in range(3):
        yb[tau] = lift(g0, tau)
    last(False, False)(0, 0)
    last(True, False)(1, 0)
    lax.fori_loop(2, 8, last(True, True), 0)
    project(lax.rem(8 * g0 + 63, 64), hb[...])
    ship(lax.rem(g0 + 6, 8))
    feed(lax.rem(g0 + 7, 8))
    collect(lax.rem(g0 + 7, 8))

    diag = lane // 8 == lax.broadcasted_iota(jnp.int32, (16, 128), 0)

    def offsets(g, carry):
        for i in range(16):
            ob[16 * g + i] = jnp.sum(jnp.where(diag, carry, 0.0), axis=0, keepdims=True)
            carry = carry + tot[16 * g + i]
        return carry
    lax.fori_loop(0, 8, offsets, x0v)
    ship(lax.rem(g0 + 7, 8))

    def small(q):
        return pltpu.make_async_remote_copy(src_ref=ob.at[q], dst_ref=offs.at[me], send_sem=sa.at[2],
                                            recv_sem=sa.at[3], device_id={"time": q}, device_id_type=MESH)

    def post(k, _):
        small(lax.rem(me + k, 128)).start()
        return 0
    lax.fori_loop(1, 128, post, 0)
    recv[me] = sb[me]
    offs[me] = ob[me]

    for k, ref in enumerate((sb.at[pl.ds(0, 127), pl.ds(0, ROWS)], recv.at[pl.ds(0, 127), pl.ds(0, ROWS)],
                             ob.at[pl.ds(0, 127)], offs.at[pl.ds(0, 127)])):
        pltpu.make_async_copy(ref, ref, sa.at[k]).wait()


def sweeps(*args):
    v = pl.BlockSpec(memory_space=pltpu.VMEM)
    h = pl.BlockSpec(memory_space=pltpu.HBM)
    dma = pltpu.SemaphoreType.DMA
    return pl.pallas_call(
        body,
        out_shape=(jax.ShapeDtypeStruct((128, 16, 128), F32), jax.ShapeDtypeStruct((128, 1, 128), F32)),
        in_specs=[h, h, pl.BlockSpec(memory_space=pltpu.SMEM), h, h, h], out_specs=(v, v),
        scratch_shapes=[
            pltpu.VMEM((128, 2, 16, 256), BF16), pltpu.VMEM((128, 1, 128), F32),
            pltpu.VMEM((10, 16, 64), F32), pltpu.VMEM((10, 256), BF16), pltpu.VMEM((10, 256), BF16),
            pltpu.VMEM((2048, 1, 256), F32), pltpu.VMEM((2048, 1, 256), F32),
            pltpu.VMEM((16, 128, 128), BF16), pltpu.VMEM((129, 16, 128), F32),
            pltpu.VMEM((128, 256), BF16), pltpu.VMEM((16, 256), BF16), pltpu.VMEM((256, 256), BF16),
            pltpu.VMEM((128, 16, 128), F32), pltpu.VMEM((128, 16, 128), F32), pltpu.VMEM((128, 1, 128), F32),
            dma((5,)), dma, dma, dma((4,)), dma((2, 4)), dma((4,)), dma((4,)), dma((3,)), dma((4,)),
            pltpu.VMEM((8, 128, 256), BF16), pltpu.VMEM((3, 128, 256), F32), pltpu.VMEM((256, 256), BF16), pltpu.VMEM((256, 256), F32),
            pltpu.VMEM((128, 256), F32), pltpu.VMEM((16, 128), F32)],
        compiler_params=pltpu.CompilerParams(vmem_limit_bytes=58 * 2**20, collective_id=0, has_side_effects=True),
    )(*args)


def untangle(src, off, out):
    for half in range(2):
        base = off[64 * half:64 * half + 64, :].T
        for c in range(10):
            m = src[half, :, c, :].T
            for k in range(16):
                out[k, c, 8 * half:8 * half + 8, :] = m[8 * k:8 * k + 8, :] + base[8 * c:8 * c + 8, :]


def solution(mesh):
    def local(x_init, w_in, w_out, mod_scale, mod_shift, step_size):
        got, off = sweeps(mod_scale, mod_shift, step_size, jnp.transpose(x_init, (2, 1, 0)), w_in, w_out.T)
        v = pl.BlockSpec(memory_space=pltpu.VMEM)
        res = pl.pallas_call(untangle, out_shape=jax.ShapeDtypeStruct((16, 10, 16, 64), F32), in_specs=[v, v], out_specs=v)(
            got.reshape(2, 64, 16, 128), off.reshape(128, 128))
        return jnp.transpose(res, (0, 3, 2, 1))

    return jax.shard_map(local, mesh=mesh, in_specs=(P("data"), P(), P(), P("time"), P("time"), P("time")), out_specs=P("time", "data"), check_vma=False)
```

```python
import functools

import jax
import jax.numpy as jnp
from jax import lax
from jax.experimental import pallas as pl
from jax.experimental.pallas import tpu as pltpu
from jax.sharding import PartitionSpec as P

MESH = pl.DeviceIdType.MESH
ROWS = 10
FEED = 9
CUBE = 0.044715
ROOT = 0.7978845608028654
F32, BF16 = jnp.float32, jnp.bfloat16

def nn(a, b):
    return lax.dot_general(a, b, (((1,), (0,)), ((), ())), preferred_element_type=F32)

def act(y):
    q = y * ((2.0 * ROOT) + (8.0 * ROOT * CUBE) * (y * y))
    return (y + y * jnp.tanh(q)).astype(BF16)


def coords(me):
    return (me // 2) % 4, (me // 8) % 4, me // 32


def gather(ms, mt, st, buf, hs, sl, ss, sh, rab, rc, rf, rd, rp, rh, ready, work):
    me = lax.axis_index("time")
    core = me % 2
    x, y, z = coords(me)
    a = x + core * (z - x)
    b = y
    c = z + core * (x - z)
    ka, kc = 1 + 15 * core, 16 - 15 * core
    base = core * 64

    def dev(da, db, dc):
        aa, bb, cc = (a + da) % 4, (b + db) % 4, (c + dc) % 4
        return 2 * (aa * ka + bb * 4 + cc * kc) + core

    def group(db, dc):
        return pl.ds(pl.multiple_of(base + ((c + dc) % 4) * 16 + ((b + db) % 4) * 4, 4), 4)

    partner = me + 1 - 2 * core
    mine = base + c * 16 + b * 4 + a
    plane = [(da, db) for db in (0, 1, 3, 2) for da in (0, 1, 3, 2) if da or db]
    peers = [dev(da, db, 0) for da, db in plane] + [dev(0, 0, 1), dev(0, 0, 3), dev(0, 0, 2), partner]

    barrier = pltpu.get_barrier_semaphore()
    for p in peers:
        pl.semaphore_signal(barrier, inc=1, device_id={"time": p}, device_id_type=MESH)
    loads = [pltpu.make_async_copy(ms, buf.at[mine, 0], sl.at[0]), pltpu.make_async_copy(mt, buf.at[mine, 1], sl.at[1])]
    for cp in loads:
        cp.start()
    lane = lax.broadcasted_iota(jnp.int32, (1, 128), 1)
    row = jnp.zeros((1, 128), F32)
    for k in range(16):
        row = jnp.where(lane // 8 == k, st[k] * (0.5 / 256.0), row)
    hs[mine] = row
    for cp in loads:
        cp.wait()
    pl.semaphore_wait(barrier, len(peers))

    def send(ref, s, r, p):
        pltpu.make_async_remote_copy(src_ref=ref, dst_ref=ref, send_sem=s, recv_sem=r,
                                     device_id={"time": p}, device_id_type=MESH).start()

    def arrive(ref, r):
        pltpu.make_async_copy(ref, ref, r).wait()

    for da, db in plane:
        send(buf.at[mine], ss, rab.at[db], dev(da, db, 0))
    for da, db in plane:
        send(hs.at[mine], sh, rh.at[0], dev(da, db, 0))
    ready()
    def run(db, dc):
        return base + ((c + dc) % 4) * 16 + ((b + db) % 4) * 4

    order = (0, 1, 3, 2)
    for db in order:
        ref = buf.at[group(4 - db, 0)]
        if db:
            arrive(ref, rab.at[db])
        else:
            arrive(buf.at[pl.ds(0, 3)], rab.at[0])
        send(ref, ss, rc.at[0, db], dev(0, 0, 1))
        send(ref, ss, rc.at[1, db], dev(0, 0, 3))
        send(ref, ss, rd.at[0], partner)
        if db != 2:
            work([run(4 - db, 0)])
    arrive(hs.at[pl.ds(0, 15)], rh.at[0])
    rows = hs.at[pl.ds(pl.multiple_of(base + c * 16, 16), 16)]
    for d in (1, 3, 2):
        send(rows, sh, rh.at[1], dev(0, 0, d))

    pc = x + core * (z - x)
    pbase = 64 - base

    def prun(k, dc):
        return pbase + ((pc + dc) % 4) * 16 + 4 * k

    work([run(2, 0)])
    arrive(buf.at[pl.ds(0, 16)], rd.at[0])
    work([prun(k, 0) for k in range(4)])
    def theirs(n):
        for k in range(2):
            arrive(buf.at[pl.ds(0, 4)], rp.at[k, n])
        q = ((b + 4 - order[n]) % 4)
        return [prun(q, 3), prun(q, 1)]

    for n, db in enumerate(order):
        up = buf.at[group(4 - db, 3)]
        arrive(up, rc.at[0, db])
        if n < 2:
            send(up, ss, rf.at[db], dev(0, 0, 1))
        send(up, ss, rp.at[0, n], partner)
        down = buf.at[group(4 - db, 1)]
        arrive(down, rc.at[1, db])
        if n >= 2:
            send(down, ss, rf.at[db], dev(0, 0, 3))
        send(down, ss, rp.at[1, n], partner)
        if n < 3:
            work([run(4 - db, 3), run(4 - db, 1)] + (theirs(n - 1) if n else []))
    arrive(hs.at[pl.ds(0, 48)], rh.at[1])
    send(hs.at[pl.ds(pl.multiple_of(base, 64), 64)], sh, rh.at[2], partner)
    for db in order:
        far = buf.at[group(4 - db, 2)]
        arrive(far, rf.at[db])
        send(far, ss, rd.at[1], partner)
    work([run(4 - order[3], 3), run(4 - order[3], 1)] + theirs(2) + [run(k, 2) for k in range(4)] + theirs(3))
    arrive(buf.at[pl.ds(0, 16)], rd.at[1])
    work([prun(k, 2) for k in range(4)])
    arrive(hs.at[pl.ds(0, 64)], rh.at[2])
    arrive(buf.at[pl.ds(0, 127)], ss)
    arrive(hs.at[pl.ds(0, 127)], sh)


def other(t):
    return (t % 4) * 16 + ((t // 4) % 4) * 4 + t // 16


def body(ms, mt, st, xh, wih, woh, recv, offs, buf, hs, xt_, w_in, w_out, sf, bf, xg, db, wi, wo, tris, sb, tot, ob,
         sl, ss, sh, rab, rc, rf, rd, rp, rh, sa, wz, yb, hb, eb, eb2, ub, x0s):
    early = [pltpu.make_async_copy(*pair, sl.at[2 + k]) for k, pair in enumerate(((xh, xt_), (wih, w_in), (woh, w_out)))]
    for cp in early:
        cp.start()
    db[128] = jnp.zeros((16, 128), F32)
    me = lax.axis_index("time")
    core = me % 2
    half, batch = me // 64, me % 64
    def prepare():
        wi[...] = jnp.zeros_like(wi)
        wo[...] = jnp.zeros_like(wo)
        wi[0:10, :] = w_in[...]
        wo[0:10, :] = w_out[...]
        lane8 = lax.broadcasted_iota(jnp.int32, (8, 128), 1)
        pick = lax.broadcasted_iota(jnp.int32, (8, 64), 1) == batch
        xr = jnp.zeros((8, 128), F32)
        for ch in range(10):
            col = jnp.sum(jnp.where(pick, xt_[ch, pl.ds(pl.multiple_of(half * 8, 8), 8), :], 0.0), axis=1, keepdims=True)
            xr = jnp.where(lane8 == ch, col, xr)
        x0v = jnp.concatenate([xr] * 16, axis=0).T[0:16, :]
        xl = jnp.concatenate([jnp.concatenate([xr, jnp.zeros((8, 128), F32)], axis=0).astype(BF16), jnp.zeros((16, 128), BF16)], axis=1)
        ri = lax.broadcasted_iota(jnp.int32, (256, 256), 0) % 128
        ci = lax.broadcasted_iota(jnp.int32, (256, 256), 1)
        cm = ci % 128
        tri = jnp.where(((ri % 8) == (cm % 8)) & ((ci >= 128) | ((ri // 8) < (cm // 8))), 256.0, 0.0).astype(BF16)
        tris[...] = tri
        u = nn(xl[:, 0:128], wi[...])[:8]
        for k in range(8):
            wz[k] = jnp.zeros((128, 256), BF16)
            wz[k, 16 * k:16 * k + 16, :] = wi[0:16, :]
        x0s[...] = x0v
        ub[...] = jnp.concatenate([u] * 16, axis=0)

    def spread(ref, r0):
        return jnp.broadcast_to(ref[pl.ds(r0, 16)], (16, 8, 256)).reshape(128, 256)

    def hidden(g, tau, y):
        r0 = g * 256 + tau * 16
        return act(y * spread(sf, r0) + spread(bf, r0))

    def put(t, d):
        db[2 * t] = d[:, :128]
        db[2 * t + 1] = d[:, 128:]

    def nt(a, b):
        return lax.dot_general(a, b, (((1,), (1,)), ((), ())), preferred_element_type=F32)

    def project(t, h):
        put(t, nt(wov, h))

    def ready():
        for cp in early:
            cp.wait()
        prepare()

    def work(runs):
        uu = ub[...]
        h = []
        blocks = [(n + k, k) for n in runs for k in range(4)]
        for q, (n, _) in enumerate(blocks):
            tree = n // 64
            idx = n - 64 * tree
            t = 2 * (idx + tree * (other(idx) - idx)) + tree
            r = pl.ds(t * 16, 16)
            sf[r, 0, :] = 0.5 + 0.5 * buf[n, 0].astype(F32)
            bf[r, 0, :] = 0.5 * buf[n, 1].astype(F32)
            h.append(act(uu * spread(sf, t * 16) + spread(bf, t * 16)))
            if q % 2:
                d = nt(wo[...], jnp.concatenate(h, axis=0))
                db[tp] = d[:, :128]
                db[t] = d[:, 128:]
                h = []
            tp = t

    lane = lax.broadcasted_iota(jnp.int32, (16, 128), 1)
    zb = jnp.zeros((16, 128), BF16)

    def feed(g, e=None):
        e = eb if e is None else e
        rolled = None
        prs = []
        for i in range(16):
            t = g * 16 + i
            tile = g * 8 + i // 2
            tile = 64 + other(tile) if i % 2 else tile
            d = db[t]
            here = pltpu.roll(d, 120, 1) if rolled is None else rolled
            rolled = pltpu.roll(db[t + 1], 120, 1)
            gr = (d + jnp.where(lane < 120, here, rolled)) * hs[tile]
            hi = gr.astype(BF16)
            r1 = gr - hi.astype(F32)
            mid = r1.astype(BF16)
            lo = (r1 - mid.astype(F32)).astype(BF16)
            prs.append((hi, mid, lo))
        cat = lambda f: jnp.concatenate([f(p) for p in prs], axis=0)
        lhs = jnp.concatenate([cat(lambda p: p[0]), cat(lambda p: p[1])], axis=1)
        e[...] = nn(lhs, tris[...]) + nn(cat(lambda p: p[2]), tris[0:128, :])

    def drain(carry, e=None):
        e = eb if e is None else e
        xs = []
        for i in range(16):
            xs.append(carry + e[16 * i:16 * i + 16, :128])
            carry = carry + e[16 * i:16 * i + 16, 128:]
        return xs, carry

    def store_x(g, xs):
        for q in range(2):
            xg[2 * g + q] = jnp.concatenate(xs[8 * q:8 * q + 8], axis=0).astype(BF16).T

    def lift(g, tau):
        return nn(xg[2 * g + tau // 8], wz[tau % 8])

    def drift(g, n, hooks={}):
        project(lax.rem(8 * g + 63, 64), hb[...])
        y = {k: yb[k] for k in range(3)}
        h = []
        for tau in range(16):
            if tau < 13:
                y[tau + 3] = lift(g, tau + 3)
            if 11 <= tau < 14:
                yb[tau - 11] = lift(n, tau - 11)
            h += [hidden(g, tau, y[tau])]
            if tau in hooks:
                hooks[tau]()
            if tau == 15:
                hb[...] = jnp.concatenate(h, axis=0)
            elif tau % 2:
                project(8 * g + tau // 2, jnp.concatenate(h, axis=0))
                h = []

    def later(i, carry):
        g = lax.rem(i, 8)
        n = lax.rem(i + 1, 8)
        carry = jnp.where(n == 0, x0v, carry)
        xs, carry = drain(carry)
        store_x(n, xs)
        feed(lax.rem(i + 2, 8))
        drift(g, n)
        return carry

    gather(ms, mt, st, buf, hs, sl, ss, sh, rab, rc, rf, rd, rp, rh, ready, work)
    x0v = x0s[...]
    wov = wo[...]
    hb[...] = jnp.zeros_like(hb)
    feed(0)
    xs, carry = drain(x0v)
    store_x(0, xs)
    feed(1)
    for tau in range(3):
        yb[tau] = lift(0, tau)
    carry = lax.fori_loop(0, 16, later, carry)
    project(63, hb[...])

    def scan(k, carry):
        for e, f, g in ((eb, eb2, 2 * k), (eb2, eb, 2 * k + 1)):
            xs, carry = drain(carry, e)
            feed(lax.rem(g + 1, 8), f)
            store_x(g, xs)
        return carry
    feed(0)
    lax.fori_loop(0, 4, scan, x0v)
    g0 = me % 8

    diag = lane // 8 == lax.broadcasted_iota(jnp.int32, (16, 128), 0)

    def strip(v):
        return jnp.sum(jnp.where(diag, v, 0.0), axis=0, keepdims=True)

    def collect(g):
        for i in range(16):
            sb[16 * g + i] = eb[16 * i:16 * i + 16, :128]
            tot[16 * g + i] = strip(eb[16 * i:16 * i + 16, 128:])

    def ship(g):
        for i in range(16):
            q = 16 * g + i

            @pl.when(q != me)
            def _():
                bulk(q).start()

    def bulk(q):
        return pltpu.make_async_remote_copy(src_ref=sb.at[q, pl.ds(0, ROWS)], dst_ref=recv.at[me, pl.ds(0, ROWS)], send_sem=sa.at[0],
                                            recv_sem=sa.at[1], device_id={"time": q}, device_id_type=MESH)

    def last(feeds, ships):
        def run(i, _):
            g = lax.rem(g0 + i, 8)
            hooks = {}
            if ships:
                hooks[2] = lambda: ship(lax.rem(g + 6, 8))
            if feeds:
                hooks[FEED] = lambda: feed(lax.rem(g + 7, 8))
            drift(g, lax.rem(g + 1, 8), hooks)
            if feeds:
                collect(lax.rem(g + 7, 8))
            return 0
        return run
    for tau in range(3):
        yb[tau] = lift(g0, tau)
    last(False, False)(0, 0)
    last(True, False)(1, 0)
    lax.fori_loop(2, 8, last(True, True), 0)
    project(lax.rem(8 * g0 + 63, 64), hb[...])
    ship(lax.rem(g0 + 6, 8))
    feed(lax.rem(g0 + 7, 8))
    collect(lax.rem(g0 + 7, 8))

    def offsets(g, carry):
        for i in range(16):
            ob[16 * g + i] = carry
            carry = carry + tot[16 * g + i]
        return carry
    lax.fori_loop(0, 8, offsets, strip(x0v))
    ship(lax.rem(g0 + 7, 8))

    def small(q):
        return pltpu.make_async_remote_copy(src_ref=ob.at[q], dst_ref=offs.at[me], send_sem=sa.at[2],
                                            recv_sem=sa.at[3], device_id={"time": q}, device_id_type=MESH)

    def post(k, _):
        small(lax.rem(me + k, 128)).start()
        return 0
    lax.fori_loop(1, 128, post, 0)
    recv[me] = sb[me]
    offs[me] = ob[me]

    for k, ref in enumerate((sb.at[pl.ds(0, 127), pl.ds(0, ROWS)], recv.at[pl.ds(0, 127), pl.ds(0, ROWS)],
                             ob.at[pl.ds(0, 127)], offs.at[pl.ds(0, 127)])):
        pltpu.make_async_copy(ref, ref, sa.at[k]).wait()


def sweeps(*args):
    v = pl.BlockSpec(memory_space=pltpu.VMEM)
    h = pl.BlockSpec(memory_space=pltpu.HBM)
    dma = pltpu.SemaphoreType.DMA
    return pl.pallas_call(
        body,
        out_shape=(jax.ShapeDtypeStruct((128, 16, 128), F32), jax.ShapeDtypeStruct((128, 1, 128), F32)),
        in_specs=[h, h, pl.BlockSpec(memory_space=pltpu.SMEM), h, h, h], out_specs=(v, v),
        scratch_shapes=[
            pltpu.VMEM((128, 2, 16, 256), BF16), pltpu.VMEM((128, 1, 128), F32),
            pltpu.VMEM((10, 16, 64), F32), pltpu.VMEM((10, 256), BF16), pltpu.VMEM((10, 256), BF16),
            pltpu.VMEM((2048, 1, 256), F32), pltpu.VMEM((2048, 1, 256), F32),
            pltpu.VMEM((16, 128, 128), BF16), pltpu.VMEM((129, 16, 128), F32),
            pltpu.VMEM((128, 256), BF16), pltpu.VMEM((16, 256), BF16), pltpu.VMEM((256, 256), BF16),
            pltpu.VMEM((128, 16, 128), F32), pltpu.VMEM((128, 1, 128), F32), pltpu.VMEM((128, 1, 128), F32),
            dma((5,)), dma, dma, dma((4,)), dma((2, 4)), dma((4,)), dma((2,)), dma((2, 4)), dma((3,)), dma((4,)),
            pltpu.VMEM((8, 128, 256), BF16), pltpu.VMEM((3, 128, 256), F32), pltpu.VMEM((256, 256), BF16), pltpu.VMEM((256, 256), F32), pltpu.VMEM((256, 256), F32),
            pltpu.VMEM((128, 256), F32), pltpu.VMEM((16, 128), F32)],
        compiler_params=pltpu.CompilerParams(vmem_limit_bytes=58 * 2**20, collective_id=0, has_side_effects=True),
    )(*args)


def untangle(src, off, out):
    for half in range(2):
        base = off[64 * half:64 * half + 64, :].T
        for c in range(10):
            m = src[half, :, c, :].T
            for k in range(16):
                out[k, c, 8 * half:8 * half + 8, :] = m[8 * k:8 * k + 8, :] + base[8 * c:8 * c + 8, :]


def solution(mesh):
    def local(x_init, w_in, w_out, mod_scale, mod_shift, step_size):
        got, off = sweeps(mod_scale, mod_shift, step_size, jnp.transpose(x_init, (2, 1, 0)), w_in, w_out.T)
        v = pl.BlockSpec(memory_space=pltpu.VMEM)
        res = pl.pallas_call(untangle, out_shape=jax.ShapeDtypeStruct((16, 10, 16, 64), F32), in_specs=[v, v], out_specs=v)(
            got.reshape(2, 64, 16, 128), off.reshape(128, 128))
        return jnp.transpose(res, (0, 3, 2, 1))

    return jax.shard_map(local, mesh=mesh, in_specs=(P("data"), P(), P(), P("time"), P("time"), P("time")), out_specs=P("time", "data"), check_vma=False)
```

```python
import functools

import jax
import jax.numpy as jnp
from jax import lax
from jax.experimental import pallas as pl
from jax.experimental.pallas import tpu as pltpu
from jax.sharding import PartitionSpec as P

MESH = pl.DeviceIdType.MESH
ROWS = 10
FEED = 9
CUBE = 0.044715
ROOT = 0.7978845608028654
F32, BF16 = jnp.float32, jnp.bfloat16

def nn(a, b):
    return lax.dot_general(a, b, (((1,), (0,)), ((), ())), preferred_element_type=F32)

def act(y):
    q = y * ((2.0 * ROOT) + (8.0 * ROOT * CUBE) * (y * y))
    return (y + y * jnp.tanh(q)).astype(BF16)


def coords(me):
    return (me // 2) % 4, (me // 8) % 4, me // 32


def gather(ms, mt, st, sv, buf, hs, sl, ss, sh, rab, rc, rf, rd, rp, rh, ready, work):
    me = lax.axis_index("time")
    core = me % 2
    x, y, z = coords(me)
    a = x + core * (z - x)
    b = y
    c = z + core * (x - z)
    ka, kc = 1 + 15 * core, 16 - 15 * core
    base = core * 64

    def dev(da, db, dc):
        aa, bb, cc = (a + da) % 4, (b + db) % 4, (c + dc) % 4
        return 2 * (aa * ka + bb * 4 + cc * kc) + core

    def group(db, dc):
        return pl.ds(pl.multiple_of(base + ((c + dc) % 4) * 16 + ((b + db) % 4) * 4, 4), 4)

    partner = me + 1 - 2 * core
    mine = base + c * 16 + b * 4 + a
    plane = [(da, db) for db in (0, 1, 3, 2) for da in (0, 1, 3, 2) if da or db]
    peers = [dev(da, db, 0) for da, db in plane] + [dev(0, 0, 1), dev(0, 0, 3), dev(0, 0, 2), partner]

    barrier = pltpu.get_barrier_semaphore()
    for p in peers:
        pl.semaphore_signal(barrier, inc=1, device_id={"time": p}, device_id_type=MESH)
    loads = [pltpu.make_async_copy(ms, buf.at[mine, 0], sl.at[0]), pltpu.make_async_copy(mt, buf.at[mine, 1], sl.at[1]),
             pltpu.make_async_copy(st, sv, sl.at[5])]
    for cp in loads:
        cp.start()
    for cp in loads:
        cp.wait()
    lane = lax.broadcasted_iota(jnp.int32, (1, 128), 1)
    row = jnp.zeros((1, 128), F32)
    for k in range(16):
        row = jnp.where(lane // 8 == k, sv[0:1, k:k + 1] * (0.5 / 256.0), row)
    hs[mine] = row
    pl.semaphore_wait(barrier, len(peers))

    def send(ref, s, r, p):
        pltpu.make_async_remote_copy(src_ref=ref, dst_ref=ref, send_sem=s, recv_sem=r,
                                     device_id={"time": p}, device_id_type=MESH).start()

    def arrive(ref, r):
        pltpu.make_async_copy(ref, ref, r).wait()

    for da, db in plane:
        send(buf.at[mine], ss, rab.at[db], dev(da, db, 0))
    for da, db in plane:
        send(hs.at[mine], sh, rh.at[0], dev(da, db, 0))
    ready()
    def run(db, dc):
        return base + ((c + dc) % 4) * 16 + ((b + db) % 4) * 4

    order = (0, 1, 3, 2)
    for db in order:
        ref = buf.at[group(4 - db, 0)]
        if db:
            arrive(ref, rab.at[db])
        else:
            arrive(buf.at[pl.ds(0, 3)], rab.at[0])
        send(ref, ss, rc.at[0, db], dev(0, 0, 1))
        send(ref, ss, rc.at[1, db], dev(0, 0, 3))
        send(ref, ss, rd.at[0], partner)
        if db != 2:
            work([run(4 - db, 0)])
    arrive(hs.at[pl.ds(0, 15)], rh.at[0])
    rows = hs.at[pl.ds(pl.multiple_of(base + c * 16, 16), 16)]
    for d in (1, 3, 2):
        send(rows, sh, rh.at[1], dev(0, 0, d))

    pc = x + core * (z - x)
    pbase = 64 - base

    def prun(k, dc):
        return pbase + ((pc + dc) % 4) * 16 + 4 * k

    work([run(2, 0)])
    arrive(buf.at[pl.ds(0, 16)], rd.at[0])
    work([prun(k, 0) for k in range(4)])
    def theirs(n):
        for k in range(2):
            arrive(buf.at[pl.ds(0, 4)], rp.at[k, n])
        q = ((b + 4 - order[n]) % 4)
        return [prun(q, 3), prun(q, 1)]

    for n, db in enumerate(order):
        up = buf.at[group(4 - db, 3)]
        arrive(up, rc.at[0, db])
        if n < 2:
            send(up, ss, rf.at[db], dev(0, 0, 1))
        send(up, ss, rp.at[0, n], partner)
        down = buf.at[group(4 - db, 1)]
        arrive(down, rc.at[1, db])
        if n >= 2:
            send(down, ss, rf.at[db], dev(0, 0, 3))
        send(down, ss, rp.at[1, n], partner)
        if n < 3:
            work([run(4 - db, 3), run(4 - db, 1)] + (theirs(n - 1) if n else []))
    arrive(hs.at[pl.ds(0, 48)], rh.at[1])
    send(hs.at[pl.ds(pl.multiple_of(base, 64), 64)], sh, rh.at[2], partner)
    for db in order:
        far = buf.at[group(4 - db, 2)]
        arrive(far, rf.at[db])
        send(far, ss, rd.at[1], partner)
    work([run(4 - order[3], 3), run(4 - order[3], 1)] + theirs(2) + [run(k, 2) for k in range(4)] + theirs(3))
    arrive(buf.at[pl.ds(0, 16)], rd.at[1])
    work([prun(k, 2) for k in range(4)])
    arrive(hs.at[pl.ds(0, 64)], rh.at[2])
    arrive(buf.at[pl.ds(0, 127)], ss)
    arrive(hs.at[pl.ds(0, 127)], sh)


def other(t):
    return (t % 4) * 16 + ((t // 4) % 4) * 4 + t // 16


def body(ms, mt, st, xh, wih, woh, recv, offs, buf, hs, xt_, w_in, w_out, sf, bf, xg, db, wi, wo, tris, sb, tot, ob,
         sl, ss, sh, rab, rc, rf, rd, rp, rh, sa, wz, yb, hb, eb, eb2, ub, x0s, sv):
    early = [pltpu.make_async_copy(*pair, sl.at[2 + k]) for k, pair in enumerate(((xh, xt_), (wih, w_in), (woh, w_out)))]
    for cp in early:
        cp.start()
    db[128] = jnp.zeros((16, 128), F32)
    me = lax.axis_index("time")
    core = me % 2
    half, batch = me // 64, me % 64
    def prepare():
        wi[...] = jnp.zeros_like(wi)
        wo[...] = jnp.zeros_like(wo)
        wi[0:10, :] = w_in[...]
        wo[0:10, :] = w_out[...]
        lane8 = lax.broadcasted_iota(jnp.int32, (8, 128), 1)
        pick = lax.broadcasted_iota(jnp.int32, (8, 64), 1) == batch
        xr = jnp.zeros((8, 128), F32)
        for ch in range(10):
            col = jnp.sum(jnp.where(pick, xt_[ch, pl.ds(pl.multiple_of(half * 8, 8), 8), :], 0.0), axis=1, keepdims=True)
            xr = jnp.where(lane8 == ch, col, xr)
        x0v = jnp.concatenate([xr] * 16, axis=0).T[0:16, :]
        xl = jnp.concatenate([jnp.concatenate([xr, jnp.zeros((8, 128), F32)], axis=0).astype(BF16), jnp.zeros((16, 128), BF16)], axis=1)
        ri = lax.broadcasted_iota(jnp.int32, (256, 256), 0) % 128
        ci = lax.broadcasted_iota(jnp.int32, (256, 256), 1)
        cm = ci % 128
        tri = jnp.where(((ri % 8) == (cm % 8)) & ((ci >= 128) | ((ri // 8) < (cm // 8))), 256.0, 0.0).astype(BF16)
        tris[...] = tri
        u = nn(xl[:, 0:128], wi[...])[:8]
        for k in range(8):
            wz[k] = jnp.zeros((128, 256), BF16)
            wz[k, 16 * k:16 * k + 16, :] = wi[0:16, :]
        x0s[...] = x0v
        ub[...] = jnp.concatenate([u] * 16, axis=0)

    def spread(ref, r0):
        return jnp.broadcast_to(ref[pl.ds(r0, 16)], (16, 8, 256)).reshape(128, 256)

    def hidden(g, tau, y):
        r0 = g * 256 + tau * 16
        return act(y * spread(sf, r0) + spread(bf, r0))

    def put(t, d):
        db[2 * t] = d[:, :128]
        db[2 * t + 1] = d[:, 128:]

    def nt(a, b):
        return lax.dot_general(a, b, (((1,), (1,)), ((), ())), preferred_element_type=F32)

    def project(t, h):
        put(t, nt(wov, h))

    def ready():
        for cp in early:
            cp.wait()
        prepare()

    def work(runs):
        uu = ub[...]
        h = []
        blocks = [(n + k, k) for n in runs for k in range(4)]
        for q, (n, _) in enumerate(blocks):
            tree = n // 64
            idx = n - 64 * tree
            t = 2 * (idx + tree * (other(idx) - idx)) + tree
            r = pl.ds(t * 16, 16)
            sf[r, 0, :] = 0.5 + 0.5 * buf[n, 0].astype(F32)
            bf[r, 0, :] = 0.5 * buf[n, 1].astype(F32)
            h.append(act(uu * spread(sf, t * 16) + spread(bf, t * 16)))
            if q % 2:
                d = nt(wo[...], jnp.concatenate(h, axis=0))
                db[tp] = d[:, :128]
                db[t] = d[:, 128:]
                h = []
            tp = t

    lane = lax.broadcasted_iota(jnp.int32, (16, 128), 1)
    zb = jnp.zeros((16, 128), BF16)

    def feed(g, e=None):
        e = eb if e is None else e
        rolled = None
        prs = []
        for i in range(16):
            t = g * 16 + i
            tile = g * 8 + i // 2
            tile = 64 + other(tile) if i % 2 else tile
            d = db[t]
            here = pltpu.roll(d, 120, 1) if rolled is None else rolled
            rolled = pltpu.roll(db[t + 1], 120, 1)
            gr = (d + jnp.where(lane < 120, here, rolled)) * hs[tile]
            hi = gr.astype(BF16)
            r1 = gr - hi.astype(F32)
            mid = r1.astype(BF16)
            lo = (r1 - mid.astype(F32)).astype(BF16)
            prs.append((hi, mid, lo))
        cat = lambda f: jnp.concatenate([f(p) for p in prs], axis=0)
        lhs = jnp.concatenate([cat(lambda p: p[0]), cat(lambda p: p[1])], axis=1)
        e[...] = nn(lhs, tris[...]) + nn(cat(lambda p: p[2]), tris[0:128, :])

    def drain(carry, e=None):
        e = eb if e is None else e
        xs = []
        for i in range(16):
            xs.append(carry + e[16 * i:16 * i + 16, :128])
            carry = carry + e[16 * i:16 * i + 16, 128:]
        return xs, carry

    def store_x(g, xs):
        for q in range(2):
            xg[2 * g + q] = jnp.concatenate(xs[8 * q:8 * q + 8], axis=0).astype(BF16).T

    def lift(g, tau):
        return nn(xg[2 * g + tau // 8], wz[tau % 8])

    def drift(g, n, hooks={}):
        project(lax.rem(8 * g + 63, 64), hb[...])
        y = {k: yb[k] for k in range(3)}
        h = []
        for tau in range(16):
            if tau < 13:
                y[tau + 3] = lift(g, tau + 3)
            if 11 <= tau < 14:
                yb[tau - 11] = lift(n, tau - 11)
            h += [hidden(g, tau, y[tau])]
            if tau in hooks:
                hooks[tau]()
            if tau == 15:
                hb[...] = jnp.concatenate(h, axis=0)
            elif tau % 2:
                project(8 * g + tau // 2, jnp.concatenate(h, axis=0))
                h = []

    def later(i, carry):
        g = lax.rem(i, 8)
        n = lax.rem(i + 1, 8)
        carry = jnp.where(n == 0, x0v, carry)
        xs, carry = drain(carry)
        store_x(n, xs)
        feed(lax.rem(i + 2, 8))
        drift(g, n)
        return carry

    gather(ms, mt, st, sv, buf, hs, sl, ss, sh, rab, rc, rf, rd, rp, rh, ready, work)
    x0v = x0s[...]
    wov = wo[...]
    hb[...] = jnp.zeros_like(hb)
    feed(0)
    xs, carry = drain(x0v)
    store_x(0, xs)
    feed(1)
    for tau in range(3):
        yb[tau] = lift(0, tau)
    carry = lax.fori_loop(0, 16, later, carry)
    project(63, hb[...])

    def scan(k, carry):
        for e, f, g in ((eb, eb2, 2 * k), (eb2, eb, 2 * k + 1)):
            xs, carry = drain(carry, e)
            feed(lax.rem(g + 1, 8), f)
            store_x(g, xs)
        return carry
    feed(0)
    lax.fori_loop(0, 4, scan, x0v)
    g0 = me % 8

    diag = lane // 8 == lax.broadcasted_iota(jnp.int32, (16, 128), 0)

    def strip(v):
        return jnp.sum(jnp.where(diag, v, 0.0), axis=0, keepdims=True)

    def collect(g):
        for i in range(16):
            sb[16 * g + i] = eb[16 * i:16 * i + 16, :128]
            tot[16 * g + i] = strip(eb[16 * i:16 * i + 16, 128:])

    def ship(g):
        for i in range(16):
            q = 16 * g + i

            @pl.when(q != me)
            def _():
                bulk(q).start()

    def bulk(q):
        return pltpu.make_async_remote_copy(src_ref=sb.at[q, pl.ds(0, ROWS)], dst_ref=recv.at[me, pl.ds(0, ROWS)], send_sem=sa.at[0],
                                            recv_sem=sa.at[1], device_id={"time": q}, device_id_type=MESH)

    def last(feeds, ships):
        def run(i, _):
            g = lax.rem(g0 + i, 8)
            hooks = {}
            if ships:
                hooks[2] = lambda: ship(lax.rem(g + 6, 8))
            if feeds:
                hooks[FEED] = lambda: feed(lax.rem(g + 7, 8))
            drift(g, lax.rem(g + 1, 8), hooks)
            if feeds:
                collect(lax.rem(g + 7, 8))
            return 0
        return run
    for tau in range(3):
        yb[tau] = lift(g0, tau)
    last(False, False)(0, 0)
    last(True, False)(1, 0)
    lax.fori_loop(2, 8, last(True, True), 0)
    project(lax.rem(8 * g0 + 63, 64), hb[...])
    ship(lax.rem(g0 + 6, 8))
    feed(lax.rem(g0 + 7, 8))
    collect(lax.rem(g0 + 7, 8))

    def offsets(g, carry):
        for i in range(16):
            ob[16 * g + i] = carry
            carry = carry + tot[16 * g + i]
        return carry
    lax.fori_loop(0, 8, offsets, strip(x0v))
    ship(lax.rem(g0 + 7, 8))

    def small(q):
        return pltpu.make_async_remote_copy(src_ref=ob.at[q], dst_ref=offs.at[me], send_sem=sa.at[2],
                                            recv_sem=sa.at[3], device_id={"time": q}, device_id_type=MESH)

    def post(k, _):
        small(lax.rem(me + k, 128)).start()
        return 0
    lax.fori_loop(1, 128, post, 0)
    recv[me] = sb[me]
    offs[me] = ob[me]

    for k, ref in enumerate((sb.at[pl.ds(0, 127), pl.ds(0, ROWS)], recv.at[pl.ds(0, 127), pl.ds(0, ROWS)],
                             ob.at[pl.ds(0, 127)], offs.at[pl.ds(0, 127)])):
        pltpu.make_async_copy(ref, ref, sa.at[k]).wait()


def sweeps(*args):
    v = pl.BlockSpec(memory_space=pltpu.VMEM)
    h = pl.BlockSpec(memory_space=pltpu.HBM)
    dma = pltpu.SemaphoreType.DMA
    return pl.pallas_call(
        body,
        out_shape=(jax.ShapeDtypeStruct((128, 16, 128), F32), jax.ShapeDtypeStruct((128, 1, 128), F32)),
        in_specs=[h] * 6, out_specs=(v, v),
        scratch_shapes=[
            pltpu.VMEM((128, 2, 16, 256), BF16), pltpu.VMEM((128, 1, 128), F32),
            pltpu.VMEM((10, 16, 64), F32), pltpu.VMEM((10, 256), BF16), pltpu.VMEM((10, 256), BF16),
            pltpu.VMEM((2048, 1, 256), F32), pltpu.VMEM((2048, 1, 256), F32),
            pltpu.VMEM((16, 128, 128), BF16), pltpu.VMEM((129, 16, 128), F32),
            pltpu.VMEM((128, 256), BF16), pltpu.VMEM((16, 256), BF16), pltpu.VMEM((256, 256), BF16),
            pltpu.VMEM((128, 16, 128), F32), pltpu.VMEM((128, 1, 128), F32), pltpu.VMEM((128, 1, 128), F32),
            dma((6,)), dma, dma, dma((4,)), dma((2, 4)), dma((4,)), dma((2,)), dma((2, 4)), dma((3,)), dma((4,)),
            pltpu.VMEM((8, 128, 256), BF16), pltpu.VMEM((3, 128, 256), F32), pltpu.VMEM((256, 256), BF16), pltpu.VMEM((256, 256), F32), pltpu.VMEM((256, 256), F32),
            pltpu.VMEM((128, 256), F32), pltpu.VMEM((16, 128), F32), pltpu.VMEM((1, 16), F32)],
        compiler_params=pltpu.CompilerParams(vmem_limit_bytes=58 * 2**20, collective_id=0, has_side_effects=True),
    )(*args)


def untangle(src, off, out):
    for half in range(2):
        base = off[64 * half:64 * half + 64, :].T
        for c in range(10):
            m = src[half, :, c, :].T
            for k in range(16):
                out[k, c, 8 * half:8 * half + 8, :] = m[8 * k:8 * k + 8, :] + base[8 * c:8 * c + 8, :]


def solution(mesh):
    def local(x_init, w_in, w_out, mod_scale, mod_shift, step_size):
        got, off = sweeps(mod_scale, mod_shift, step_size.reshape(1, 16), jnp.transpose(x_init, (2, 1, 0)), w_in, w_out.T)
        v = pl.BlockSpec(memory_space=pltpu.VMEM)
        res = pl.pallas_call(untangle, out_shape=jax.ShapeDtypeStruct((16, 10, 16, 64), F32), in_specs=[v, v], out_specs=v)(
            got.reshape(2, 64, 16, 128), off.reshape(128, 128))
        return jnp.transpose(res, (0, 3, 2, 1))

    return jax.shard_map(local, mesh=mesh, in_specs=(P("data"), P(), P(), P("time"), P("time"), P("time")), out_specs=P("time", "data"), check_vma=False)
```
